256 devices in a mesh: layout: 2 (over z), tile: 64 (over x, y), chan: 2 (over core).
Axes of the slice: x: 8, y: 8, z: 2, core: 2. Of those that a mesh axis runs over, the one named last changes fastest.
The devices are a block of a 8x8x16 slice.
Arguments:
- sample_weight: float32 [256, 64, 256], P(('layout', 'tile', 'chan')), parts along dimension 0, may hold values from 0.25 to 4
- fraction_u: float32 [256, 64, 256], P(('layout', 'tile', 'chan')), parts along dimension 0, may hold values from 0 to 1
- fraction_v: float32 [256, 64, 256], P(('layout', 'tile', 'chan')), parts along dimension 0, may hold values from 0 to 1
- cell_code: int32 [256, 64, 256], P(('layout', 'tile', 'chan')), parts along dimension 0, may hold values from 260 to 3835, as said below
- tile_fill: int32 [256, 64, 64], P(('layout', 'tile', 'chan')), parts along dimension 0, may hold values from 0 to 4, as said below
Outputs:
- psf: float32 [8192, 4096], P(('layout', 'tile', 'chan')), parts along dimension 0
The draws below stay inside these ranges and needn't reach their ends.
There are 2 independent parts, one for each index of `layout`. The reference program is written for one: setup_inputs(seed, part) draws one part's arguments, and reference() takes and returns one part's arrays. A program takes and returns all parts, laid end to end along the dimension named above; each array names one. Nothing has to cross between parts.
Inputs may be any that keep to these rules, and one draw needn't show every extreme that they name: `cell_code`: row offset and column offset each lie in 4 .. 59. `tile_fill`: some uv tile is full from every sender; tiles near the grid's centre hold more samples than outer ones.
All inputs are finite; a program needn't handle non-finite values.
Results may differ from the reference program's by a relative error of at most 0.0003.
Values sent between devices are 32-bit elements; how exact they have to be, the bound alone decides.
A program may use at most 64 MiB of HBM per device.

```python
import math
import jax
import jax.numpy as jnp
from jax import lax

G = 4096
TILE = 64
HALF = 3
CAP = 4
NT = 64
SENDERS = 128
N_TILE = 64
N_CHAN = 2


def draw_cell_code(key, part):
    key_row = jax.random.fold_in(key, 11)
    key_col = jax.random.fold_in(key, 12)
    shape = (SENDERS, NT, NT * CAP)
    row_off = jax.random.randint(key_row, shape, HALF + 1, TILE - HALF - 1, dtype=jnp.int32)
    col_off = jax.random.randint(key_col, shape, HALF + 1, TILE - HALF - 1, dtype=jnp.int32)
    return row_off * TILE + col_off


def draw_tile_fill(key, part):
    middle = NT // 2
    tile_rows = jnp.arange(NT, dtype=jnp.int32)[:, None]
    tile_cols = jnp.arange(NT, dtype=jnp.int32)[None, :]
    radius_sq = (tile_rows - middle) * (tile_rows - middle) + (tile_cols - middle) * (tile_cols - middle)
    reach = 2 * middle * middle + 1
    limit = CAP - CAP * radius_sq // reach
    lower = limit // 2
    raw_bits = jax.random.randint(jax.random.fold_in(key, 21), (SENDERS, NT, NT), 0, 1 << 20, dtype=jnp.int32)
    filled = lower[None, :, :] + raw_bits % (limit[None, :, :] - lower[None, :, :] + 1)
    return filled.at[:, middle, middle].set(CAP)


def levels(stream_key, shape, split, low, largest):
    loudness, own = 1.0, jax.random.fold_in(stream_key, 6)
    for dim, blocks in split:
        heights = jnp.exp(jax.random.uniform(jax.random.fold_in(own, dim), (blocks,), jnp.float32, low / len(split), largest / len(split)))
        loudness = loudness * jnp.repeat(heights, shape[dim] // blocks).reshape([-1 if axis == dim else 1 for axis in range(len(shape))])
    return loudness


def setup_inputs(seed: int = 0, part: int = 0) -> dict:
    key_of = jax.random.split(jax.random.key(seed), 6)
    part_splits = jax.random.split(jax.random.fold_in(key_of[5], part), 6)
    sample_weight = jnp.clip(jnp.exp(math.log(4.0) - 2.7725887 * jax.random.uniform(part_splits[0], (SENDERS, NT, NT * CAP), jnp.float32) ** levels(part_splits[0], (SENDERS, NT, NT * CAP), ((0, 128),), -0.2, 0.2)), 0.25, 4.0)
    fraction_u = jnp.clip(1.0 * jax.random.uniform(part_splits[1], (SENDERS, NT, NT * CAP), jnp.float32) ** levels(part_splits[1], (SENDERS, NT, NT * CAP), ((0, 128),), -0.2, 0.2), 0.0, 1.0)
    fraction_v = jnp.clip(1.0 * jax.random.uniform(part_splits[2], (SENDERS, NT, NT * CAP), jnp.float32) ** levels(part_splits[2], (SENDERS, NT, NT * CAP), ((0, 128),), -0.2, 0.2), 0.0, 1.0)
    cell_code = draw_cell_code(jax.random.fold_in(jax.random.fold_in(key_of[5], part), 71), part)
    tile_fill = draw_tile_fill(jax.random.fold_in(jax.random.fold_in(key_of[5], part), 71), part)
    return dict(sample_weight=sample_weight, fraction_u=fraction_u, fraction_v=fraction_v, cell_code=cell_code, tile_fill=tile_fill)


def taper(distance):
    scaled = distance / (HALF + 1.0)
    inner = 1.0 - scaled * scaled
    return jnp.where(inner > 0.0, inner * inner, 0.0 * inner)

def reference(sample_weight, fraction_u, fraction_v, cell_code, tile_fill):
    senders = sample_weight.shape[0]
    ftype = sample_weight.dtype
    cell_pos = jnp.arange(TILE).astype(ftype)
    slot_index = jnp.arange(CAP, dtype=jnp.int32)

    def one_row(row):
        weight_row = sample_weight[:, row].reshape(senders, NT, CAP)
        frac_row_u = fraction_u[:, row].reshape(senders, NT, CAP)
        frac_row_v = fraction_v[:, row].reshape(senders, NT, CAP)
        code_row = cell_code[:, row].reshape(senders, NT, CAP)
        fill_row = tile_fill[:, row]
        is_live = slot_index[None, None, :] < fill_row[:, :, None]
        live_weight = jnp.where(is_live, weight_row, 0.0 * weight_row)
        row_off = (code_row // TILE).astype(ftype) + frac_row_u
        col_off = (code_row % TILE).astype(ftype) + frac_row_v
        kernel_u = taper(cell_pos - row_off[..., None]) * live_weight[..., None]
        kernel_v = taper(cell_pos - col_off[..., None])
        tiles = jnp.einsum('sncu,sncv->unv', kernel_u, kernel_v, precision=lax.Precision.HIGHEST)
        return tiles.reshape(TILE, G)
    grid = lax.map(one_row, jnp.arange(NT, dtype=jnp.int32)).reshape(G, G)
    norm_scale = 1.0 / math.sqrt(N_TILE * N_CHAN * NT * NT * CAP)
    image = jnp.real(jnp.fft.ifft2(grid)) * (float(G) * float(G) * norm_scale)
    return jnp.transpose(image).astype(jnp.float32)
```

```python
import functools
import math

import jax
import jax.numpy as jnp
import numpy as np
from jax import lax
from jax.experimental import pallas as pl
from jax.experimental.pallas import tpu as pltpu
from jax.sharding import PartitionSpec as P

G = 4096
TILE = 64
CAP = 4
NT = 64
LANES = 128
QUARTERS = 4
ROWS = TILE // QUARTERS
BLOCKS = G // LANES
OUT_ROWS = 32
MESH = pl.DeviceIdType.MESH
F32 = jnp.float32
BF16 = jnp.bfloat16


def two_parts(table):
    table = np.asarray(table, np.float32)
    high = table.astype(BF16)
    low = (table - high.astype(np.float32)).astype(BF16)
    return np.concatenate([high, low], axis=0)


@functools.lru_cache
def tables(devices):
    spread = (np.arange(NT)[:, None] == np.arange(NT * CAP)[None, :] // CAP).astype(BF16)
    turn = 2.0 * np.pi * np.outer(np.arange(LANES), np.arange(LANES)) / LANES
    cos, sin = np.cos(turn), np.sin(turn)
    row_table = two_parts(np.block([[cos, -sin], [sin, cos]]))
    turn = 2.0 * np.pi * np.outer(np.arange(BLOCKS), np.arange(LANES)) / G
    row_twist = np.stack([np.cos(turn), np.sin(turn)]).astype(np.float32)
    wide = G // ROWS
    turn = 2.0 * np.pi * np.outer(np.arange(wide), np.arange(devices)) / wide
    cos, sin = np.cos(turn), np.sin(turn)
    col_table = two_parts(np.block([[cos, -sin], [sin, cos]]))
    turn = 2.0 * np.pi * np.outer(np.arange(wide), np.arange(LANES) % ROWS) / G
    col_twist = np.stack([np.cos(turn), np.sin(turn)]).astype(np.float32)
    group = LANES // ROWS
    out_index = np.arange(ROWS * group)
    lane = np.arange(LANES)
    same = (out_index[:, None] % group == lane[None, :] // ROWS) / math.sqrt(devices * NT * NT * CAP)
    turn = 2.0 * np.pi * np.outer(out_index // group, lane % ROWS) / ROWS
    last_table = two_parts(np.concatenate([same * np.cos(turn), -same * np.sin(turn)], axis=1))
    return spread, row_table, row_twist, col_table, col_twist, last_table


def split(value):
    high = value.astype(BF16)
    return high, (value - high.astype(F32)).astype(BF16)


def dot(left, right, right_dim):
    return lax.dot_general(left, right, (((1,), (right_dim,)), ((), ())), preferred_element_type=F32)


def table_dot(table, value, right_dim):
    high, low = split(value)
    half = table.shape[0] // 2
    both = dot(table[...], high, right_dim)
    return both[:half] + both[half:] + dot(table[:half], low, right_dim)


def times(value, real, imag):
    v_re, v_im = value
    if abs(imag) < 1e-12:
        if abs(real - 1.0) < 1e-12:
            return value
        return v_re * real, None if v_im is None else v_im * real
    if v_im is None:
        return (None if abs(real) < 1e-12 else v_re * real), v_re * imag
    if abs(real) < 1e-12:
        return -v_im * imag, v_re * imag
    return v_re * real - v_im * imag, v_re * imag + v_im * real


def plus(a, b, sign):
    if b is None:
        return a
    if a is None:
        return b if sign > 0 else -b
    return a + b if sign > 0 else a - b


def real_transform(values):
    count = len(values)
    if count == 1:
        return [(values[0], None)]
    if count == 2:
        return [(values[0] + values[1], None), (values[0] - values[1], None)]
    even, odd = real_transform(values[0::2]), real_transform(values[1::2])
    out = [None] * (count // 2 + 1)
    for k in range(count // 4 + 1):
        turn = 2.0 * math.pi * k / count
        turned = times(odd[k], math.cos(turn), math.sin(turn))
        out[k] = (plus(even[k][0], turned[0], 1), plus(even[k][1], turned[1], 1))
        far_im = plus(even[k][1], turned[1], -1)
        out[count // 2 - k] = (plus(even[k][0], turned[0], -1), None if far_im is None else -far_im)
    return out


def kernel(
    tiles,
    chans,
    weight,
    frac_u,
    frac_v,
    code,
    fill,
    spread,
    row_table,
    row_twist,
    col_table,
    col_twist,
    last_table,
    out,
    sample,
    packed,
    landed,
    sorted_,
    slab,
    rows,
    high,
    low,
    spectrum,
    columns,
    send_a,
    recv_a,
    send_x,
    recv_x,
    send_b,
    recv_b,
):
    count = tiles * chans
    layout = lax.axis_index("layout")
    me = lax.axis_index("tile") * chans + lax.axis_index("chan")
    mine = lax.rem(me, QUARTERS)

    def place(index):
        return (layout, lax.div(index, chans), lax.rem(index, chans))

    def peer(step):
        return lax.rem(me + step, count)

    def await_bytes(ref, sem):
        pltpu.make_async_copy(ref, ref, sem).wait()

    barrier = pltpu.get_barrier_semaphore()

    @pl.loop(1, count)
    def _(step):
        pl.semaphore_signal(barrier, inc=1, device_id=place(peer(step)), device_id_type=MESH)

    fill_wide = dot(fill[0].astype(F32).astype(BF16), spread[...], 0)
    slot = lax.broadcasted_iota(jnp.int32, (NT, NT * CAP), 1) % CAP
    sample[0] = jnp.where(slot.astype(F32) < fill_wide, weight[0], 0.0)
    far = lax.broadcasted_iota(jnp.int32, (NT, NT * CAP), 0) >= NT // 2
    for part, position in (
        (1, (code[0] >> 6).astype(F32) + frac_u[0]),
        (2, (code[0] & (TILE - 1)).astype(F32) + frac_v[0]),
    ):
        sample[part] = jnp.where(far, TILE - position, position) * 0.25

    lower = lax.broadcasted_iota(jnp.int32, (1, LANES), 1) < LANES // 2

    @pl.loop(0, NT // 2)
    def _(p):
        for part in range(3):
            near = sample[part, pl.ds(p, 1), :]
            away = sample[part, pl.ds(NT - 1 - p, 1), :]
            for q in range(QUARTERS):
                a = near[:, (q // 2) * LANES : (q // 2 + 1) * LANES]
                b = away[:, (1 - q // 2) * LANES : (2 - q // 2) * LANES]
                if q % 2 == 0:
                    row = jnp.where(lower, a, b)
                else:
                    row = pltpu.roll(jnp.where(lower, b, a), LANES // 2, 1)
                packed[QUARTERS * p + q, pl.ds(part, 1), :] = row

    pl.semaphore_wait(barrier, count - 1)

    @pl.loop(1, count)
    def _(step):
        to = peer(step)
        pltpu.make_async_remote_copy(
            src_ref=packed.at[to],
            dst_ref=landed.at[me],
            send_sem=send_a,
            recv_sem=recv_a,
            device_id=place(to),
            device_id_type=MESH,
        ).start()

    landed[me] = packed[me]
    await_bytes(landed.at[pl.ds(0, count - 1)], recv_a)

    for part in range(3):
        sorted_[part] = landed[:, part, :].T

    cell = lax.broadcasted_iota(jnp.int32, (TILE, count), 0).astype(F32) * 0.25

    def taper(row, where):
        scaled = cell - row[where]
        inner = jnp.maximum(1.0 - scaled * scaled, 0.0)
        return inner * inner

    def one_tile(k):
        total = jnp.zeros((2 * TILE, 2 * TILE), F32)
        starts = [CAP * k, NT * CAP // 2 - CAP - CAP * k]
        for start in starts:
            for pair in range(CAP // 2):
                lefts, rights = [], []
                for slot in range(2):
                    where = pl.ds(start + 2 * pair + slot, 1)
                    u_high, u_low = split(taper(sorted_.at[1], where) * sorted_[0, where])
                    v_high, v_low = split(taper(sorted_.at[2], where))
                    lefts.append(jnp.concatenate([u_high, u_low], axis=0))
                    rights.append(jnp.concatenate([v_high, v_low], axis=0))
                total += dot(jnp.concatenate(lefts, axis=1), jnp.concatenate(rights, axis=1), 1)
        return total[:TILE] + total[TILE:]

    upper_half = lax.broadcasted_iota(jnp.int32, (TILE, LANES), 1) >= TILE

    @pl.loop(0, NT // QUARTERS // 2)
    def _(pair):
        first, second = one_tile(2 * pair), one_tile(2 * pair + 1)
        first = first + pltpu.roll(first, TILE, 1)
        second = second + pltpu.roll(second, TILE, 1)
        slab[pair] = jnp.where(upper_half, second, first)

    strip = BLOCKS // QUARTERS
    for hop in range(1, QUARTERS):
        other = lax.rem(mine + hop, QUARTERS)
        pltpu.make_async_remote_copy(
            src_ref=slab.at[:, pl.ds(pl.multiple_of(other * ROWS, ROWS), ROWS), :],
            dst_ref=rows.at[pl.ds(mine * strip, strip)],
            send_sem=send_x,
            recv_sem=recv_x,
            device_id=place(me - mine + other),
            device_id_type=MESH,
        ).start()
    rows[pl.ds(mine * strip, strip)] = slab[:, pl.ds(pl.multiple_of(mine * ROWS, ROWS), ROWS), :]
    await_bytes(rows.at[pl.ds(0, BLOCKS - strip)], recv_x)

    waves = real_transform([rows[t] for t in range(BLOCKS)])
    for k in range(BLOCKS):
        re, im = waves[min(k, BLOCKS - k)]
        c, s = row_twist[0, k : k + 1, :], row_twist[1, k : k + 1, :]
        if im is None:
            turned = (re * c, re * s)
        elif k <= BLOCKS // 2:
            turned = (re * c - im * s, re * s + im * c)
        else:
            turned = (re * c + im * s, re * s - im * c)
        for part in range(2):
            upper, rest = split(turned[part])
            high[ROWS * k : ROWS * (k + 1), LANES * part : LANES * (part + 1)] = upper
            low[ROWS * k : ROWS * (k + 1), LANES * part : LANES * (part + 1)] = rest
    groups = BLOCKS * ROWS // LANES
    for lane in range(0, groups, 2):
        where = slice(LANES * lane, LANES * (lane + 2))
        both = dot(row_table[...], high[where], 1)
        half = 2 * LANES
        both = both[:half] + both[half:] + dot(row_table[:half], low[where], 1)
        for part in range(2):
            for extra in range(2):
                spectrum[pl.ds(part * groups + lane + extra, count, stride=2 * groups), :] = both[
                    part * LANES : (part + 1) * LANES, extra * LANES : (extra + 1) * LANES
                ]

    each = 2 * groups

    def block(ref, index):
        return ref.at[pl.ds(pl.multiple_of(index * each, each), each), :]

    @pl.loop(1, count)
    def _(step):
        to = peer(step)
        pltpu.make_async_remote_copy(
            src_ref=block(spectrum, to),
            dst_ref=block(columns, me),
            send_sem=send_b,
            recv_sem=recv_b,
            device_id=place(to),
            device_id_type=MESH,
        ).start()

    own = pl.ds(pl.multiple_of(me * each, each), each)
    columns[own, :] = spectrum[own, :]
    await_bytes(columns.at[pl.ds(0, (count - 1) * each), :], recv_b)

    wide = G // ROWS
    for lane in range(groups):
        real = columns[pl.ds(lane, count, stride=each), :]
        imag = columns[pl.ds(groups + lane, count, stride=each), :]
        first = table_dot(col_table, jnp.concatenate([real, imag], axis=0), 0)
        re, im = first[:wide], first[wide:]
        c, s = col_twist[0], col_twist[1]
        turned = jnp.concatenate([re * c - im * s, re * s + im * c], axis=1)
        last = table_dot(last_table, turned, 1)
        tall = LANES // ROWS
        for l2 in range(ROWS):
            out[tall * lane : tall * (lane + 1), wide * l2 : wide * (l2 + 1)] = last[tall * l2 : tall * (l2 + 1)]

    await_bytes(packed.at[pl.ds(0, count - 1)], send_a)
    await_bytes(rows.at[pl.ds(0, BLOCKS - strip)], send_x)
    await_bytes(columns.at[pl.ds(0, (count - 1) * each), :], send_b)


def body(sample_weight, fraction_u, fraction_v, cell_code, tile_fill):
    tiles, chans = lax.axis_size("tile"), lax.axis_size("chan")
    count = tiles * chans
    constants = [jnp.asarray(table) for table in tables(count)]
    return pl.pallas_call(
        functools.partial(kernel, tiles, chans),
        out_shape=jax.ShapeDtypeStruct((OUT_ROWS, G), F32),
        in_specs=[pl.BlockSpec(memory_space=pltpu.VMEM)] * (5 + len(constants)),
        out_specs=pl.BlockSpec(memory_space=pltpu.VMEM),
        scratch_shapes=[
            pltpu.VMEM((3, NT, NT * CAP), F32),
            pltpu.VMEM((count, 3, LANES), F32),
            pltpu.VMEM((count, 3, LANES), F32),
            pltpu.VMEM((3, LANES, count), F32),
            pltpu.VMEM((BLOCKS // QUARTERS, TILE, LANES), F32),
            pltpu.VMEM((BLOCKS, ROWS, LANES), F32),
            pltpu.VMEM((BLOCKS * ROWS, 2 * LANES), BF16),
            pltpu.VMEM((BLOCKS * ROWS, 2 * LANES), BF16),
            pltpu.VMEM((count * 8, LANES), F32),
            pltpu.VMEM((count * 8, LANES), F32),
        ]
        + [pltpu.SemaphoreType.DMA] * 6,
        compiler_params=pltpu.CompilerParams(collective_id=0, has_side_effects=True),
    )(sample_weight, fraction_u, fraction_v, cell_code, tile_fill, *constants)


def solution(mesh):
    spec = P(("layout", "tile", "chan"), None, None)
    return jax.shard_map(
        body,
        mesh=mesh,
        in_specs=(spec,) * 5,
        out_specs=P(("layout", "tile", "chan"), None),
        check_vma=False,
    )
```

```python
import functools
import math

import jax
import jax.numpy as jnp
import numpy as np
from jax import lax
from jax.experimental import pallas as pl
from jax.experimental.pallas import tpu as pltpu
from jax.sharding import PartitionSpec as P

G = 4096
TILE = 64
CAP = 4
NT = 64
LANES = 128
QUARTERS = 4
ROWS = TILE // QUARTERS
BLOCKS = G // LANES
OUT_ROWS = 32
MESH = pl.DeviceIdType.MESH
F32 = jnp.float32
BF16 = jnp.bfloat16


def two_parts(table):
    table = np.asarray(table, np.float32)
    high = table.astype(BF16)
    low = (table - high.astype(np.float32)).astype(BF16)
    return np.concatenate([high, low], axis=0)


@functools.lru_cache
def tables(devices):
    spread = (np.arange(NT)[:, None] == np.arange(NT * CAP)[None, :] // CAP).astype(BF16)
    turn = 2.0 * np.pi * np.outer(np.arange(LANES), np.arange(LANES)) / LANES
    cos, sin = np.cos(turn), np.sin(turn)
    row_table = two_parts(np.block([[cos, -sin], [sin, cos]]))
    turn = 2.0 * np.pi * np.outer(np.arange(BLOCKS), np.arange(LANES)) / G
    row_twist = np.stack([np.cos(turn), np.sin(turn)]).astype(np.float32)
    wide = G // ROWS
    turn = 2.0 * np.pi * np.outer(np.arange(wide), np.arange(devices)) / wide
    cos, sin = np.cos(turn), np.sin(turn)
    col_table = two_parts(np.block([[cos, -sin], [sin, cos]]))
    turn = 2.0 * np.pi * np.outer(np.arange(wide), np.arange(LANES) % ROWS) / G
    col_twist = np.stack([np.cos(turn), np.sin(turn)]).astype(np.float32)
    group = LANES // ROWS
    out_index = np.arange(ROWS * group)
    lane = np.arange(LANES)
    same = (out_index[:, None] % group == lane[None, :] // ROWS) / math.sqrt(devices * NT * NT * CAP)
    turn = 2.0 * np.pi * np.outer(out_index // group, lane % ROWS) / ROWS
    last_table = two_parts(np.concatenate([same * np.cos(turn), -same * np.sin(turn)], axis=1))
    return spread, row_table, row_twist, col_table, col_twist, last_table


def split(value):
    high = value.astype(BF16)
    return high, (value - high.astype(F32)).astype(BF16)


def dot(left, right, right_dim):
    return lax.dot_general(left, right, (((1,), (right_dim,)), ((), ())), preferred_element_type=F32)


def table_dot(table, value, right_dim):
    high, low = split(value)
    half = table.shape[0] // 2
    both = dot(table[...], high, right_dim)
    return both[:half] + both[half:] + dot(table[:half], low, right_dim)


def times(value, real, imag):
    v_re, v_im = value
    if abs(imag) < 1e-12:
        if abs(real - 1.0) < 1e-12:
            return value
        return v_re * real, None if v_im is None else v_im * real
    if v_im is None:
        return (None if abs(real) < 1e-12 else v_re * real), v_re * imag
    if abs(real) < 1e-12:
        return -v_im * imag, v_re * imag
    return v_re * real - v_im * imag, v_re * imag + v_im * real


def plus(a, b, sign):
    if b is None:
        return a
    if a is None:
        return b if sign > 0 else -b
    return a + b if sign > 0 else a - b


def real_transform(values):
    count = len(values)
    if count == 1:
        return [(values[0], None)]
    if count == 2:
        return [(values[0] + values[1], None), (values[0] - values[1], None)]
    even, odd = real_transform(values[0::2]), real_transform(values[1::2])
    out = [None] * (count // 2 + 1)
    for k in range(count // 4 + 1):
        turn = 2.0 * math.pi * k / count
        turned = times(odd[k], math.cos(turn), math.sin(turn))
        out[k] = (plus(even[k][0], turned[0], 1), plus(even[k][1], turned[1], 1))
        far_im = plus(even[k][1], turned[1], -1)
        out[count // 2 - k] = (plus(even[k][0], turned[0], -1), None if far_im is None else -far_im)
    return out


def kernel(tiles, chans, *refs):
    inputs, tables_in, refs = refs[:5], refs[5:11], refs[11:]
    out, refs = refs[0], refs[1:]
    weight, frac_u, frac_v, code, fill = refs[:5]
    spread, row_table, row_twist, col_table, col_twist, last_table = refs[5:11]
    sample, packed, middle, landed, sorted_, slab, rows, high, low, spectrum, columns = refs[11:22]
    load, send_1, recv_1, send_2, recv_2, send_x, recv_x, send_b, recv_b = refs[22:]
    side = math.isqrt(tiles)
    count = tiles * chans
    line = side * chans
    layout, tile, chan = lax.axis_index("layout"), lax.axis_index("tile"), lax.axis_index("chan")
    x, y = lax.div(tile, side), lax.rem(tile, side)
    in_line = x * chans + chan
    me = tile * chans + chan
    mine = lax.rem(me, QUARTERS)
    far_first = sorted(range(side), key=lambda d: -min(d, side - d))

    def ahead(value, step):
        value = value + step
        return jnp.where(value >= side, value - side, value)

    def behind(value, step):
        value = value - step
        return jnp.where(value < 0, value + side, value)

    def place(to_x, to_y, to_chan):
        return (layout, to_x * side + to_y, to_chan)

    def send(src, dst, send_sem, recv_sem, device):
        pltpu.make_async_remote_copy(
            src_ref=src,
            dst_ref=dst,
            send_sem=send_sem,
            recv_sem=recv_sem,
            device_id=device,
            device_id_type=MESH,
        ).start()

    def await_bytes(ref, sem):
        pltpu.make_async_copy(ref, ref, sem).wait()

    line_peers = [
        (ahead(x, dx), chan if e == 0 else 1 - chan) for dx in far_first for e in range(chans) if (dx, e) != (0, 0)
    ]
    column_peers = [ahead(y, dy) for dy in far_first if dy != 0]
    barrier = pltpu.get_barrier_semaphore()
    for to_x, to_chan in line_peers:
        pl.semaphore_signal(barrier, inc=1, device_id=place(to_x, y, to_chan), device_id_type=MESH)
    for to_y in column_peers:
        pl.semaphore_signal(barrier, inc=1, device_id=place(x, to_y, chan), device_id_type=MESH)

    loads = [
        pltpu.make_async_copy(src, dst, load.at[k])
        for k, (src, dst) in enumerate(zip([*inputs, *tables_in], refs[:11], strict=True))
    ]
    for k in (4, 5, 0, 3, 1, 2, 6, 7, 8, 9, 10):
        loads[k].start()
    for k in range(6):
        loads[k].wait()

    fill_wide = dot(fill[0].astype(F32).astype(BF16), spread[...], 0)
    slot = lax.broadcasted_iota(jnp.int32, (NT, NT * CAP), 1) % CAP
    sample[0] = jnp.where(slot.astype(F32) < fill_wide, weight[0], 0.0)
    far = lax.broadcasted_iota(jnp.int32, (NT, NT * CAP), 0) >= NT // 2
    for part, position in (
        (1, (code[0] >> 6).astype(F32) + frac_u[0]),
        (2, (code[0] & (TILE - 1)).astype(F32) + frac_v[0]),
    ):
        sample[part] = jnp.where(far, TILE - position, position) * 0.25

    lower = lax.broadcasted_iota(jnp.int32, (1, LANES), 1) < LANES // 2

    @pl.loop(0, side)
    def _(to_x):
        for near_y in range(side // 2):
            p = to_x * (side // 2) + near_y
            for part in range(3):
                near = sample[part, pl.ds(p, 1), :]
                away = sample[part, pl.ds(NT - 1 - p, 1), :]
                for q in range(QUARTERS):
                    a = near[:, (q // 2) * LANES : (q // 2 + 1) * LANES]
                    b = away[:, (1 - q // 2) * LANES : (2 - q // 2) * LANES]
                    if q % 2 == 0:
                        row = jnp.where(lower, a, b)
                    else:
                        row = pltpu.roll(jnp.where(lower, b, a), LANES // 2, 1)
                    to_y, to_chan = 2 * near_y + q // 2, q % 2
                    packed[(to_x * chans + to_chan) * side + to_y, pl.ds(part, 1), :] = row

    pl.semaphore_wait(barrier, len(line_peers) + len(column_peers))

    for to_x, to_chan in line_peers:
        send(
            packed.at[pl.ds((to_x * chans + to_chan) * side, side)],
            middle.at[:, in_line],
            send_1,
            recv_1,
            place(to_x, y, to_chan),
        )
    middle[:, in_line] = packed[pl.ds(in_line * side, side)]
    await_bytes(packed.at[pl.ds(0, (line - 1) * side)], recv_1)
    for to_y in column_peers:
        send(middle.at[to_y], landed.at[y], send_2, recv_2, place(x, to_y, chan))
    landed[y] = middle[y]
    await_bytes(landed.at[pl.ds(0, side - 1)], recv_2)

    for part in range(3):
        sorted_[part] = landed[:, :, part, :].reshape(count, LANES).T

    cell = lax.broadcasted_iota(jnp.int32, (TILE, count), 0).astype(F32) * 0.25

    def taper(row, where):
        scaled = cell - row[where]
        inner = jnp.maximum(1.0 - scaled * scaled, 0.0)
        return inner * inner

    def one_tile(k):
        total = jnp.zeros((2 * TILE, 2 * TILE), F32)
        starts = [CAP * k, NT * CAP // 2 - CAP - CAP * k]
        for start in starts:
            for pair in range(CAP // 2):
                lefts, rights = [], []
                for slot in range(2):
                    where = pl.ds(start + 2 * pair + slot, 1)
                    u_high, u_low = split(taper(sorted_.at[1], where) * sorted_[0, where])
                    v_high, v_low = split(taper(sorted_.at[2], where))
                    lefts.append(jnp.concatenate([u_high, u_low], axis=0))
                    rights.append(jnp.concatenate([v_high, v_low], axis=0))
                total += dot(jnp.concatenate(lefts, axis=1), jnp.concatenate(rights, axis=1), 1)
        return total[:TILE] + total[TILE:]

    upper_half = lax.broadcasted_iota(jnp.int32, (TILE, LANES), 1) >= TILE
    strip = BLOCKS // QUARTERS
    others = []
    for hop in range(1, QUARTERS):
        other = lax.rem(mine + hop, QUARTERS)
        index = me - mine + other
        others.append((other, (layout, lax.div(index, chans), lax.rem(index, chans))))

    def row_range(index):
        return pl.ds(pl.multiple_of(index * ROWS, ROWS), ROWS)

    @pl.loop(0, strip)
    def _(pair):
        first, second = one_tile(2 * pair), one_tile(2 * pair + 1)
        first = first + pltpu.roll(first, TILE, 1)
        second = second + pltpu.roll(second, TILE, 1)
        slab[pair] = jnp.where(upper_half, second, first)
        for other, device in others:
            send(slab.at[pair, row_range(other), :], rows.at[mine * strip + pair], send_x, recv_x, device)

    rows[pl.ds(mine * strip, strip)] = slab[:, row_range(mine), :]
    for k in (6, 7):
        loads[k].wait()
    await_bytes(rows.at[pl.ds(0, BLOCKS - strip)], recv_x)

    waves = real_transform([rows[t] for t in range(BLOCKS)])
    for k in range(BLOCKS):
        re, im = waves[min(k, BLOCKS - k)]
        c, s = row_twist[0, k : k + 1, :], row_twist[1, k : k + 1, :]
        if im is None:
            turned = (re * c, re * s)
        elif k <= BLOCKS // 2:
            turned = (re * c - im * s, re * s + im * c)
        else:
            turned = (re * c + im * s, re * s - im * c)
        for part in range(2):
            upper, rest = split(turned[part])
            high[ROWS * k : ROWS * (k + 1), LANES * part : LANES * (part + 1)] = upper
            low[ROWS * k : ROWS * (k + 1), LANES * part : LANES * (part + 1)] = rest
    groups = BLOCKS * ROWS // LANES
    for lane in range(0, groups, 2):
        where = slice(LANES * lane, LANES * (lane + 2))
        both = dot(row_table[...], high[where], 1)
        half = 2 * LANES
        both = both[:half] + both[half:] + dot(row_table[:half], low[where], 1)
        for part in range(2):
            for extra in range(2):
                spectrum[pl.ds(part * groups + lane + extra, count, stride=2 * groups), :] = both[
                    part * LANES : (part + 1) * LANES, extra * LANES : (extra + 1) * LANES
                ]

    each = 2 * groups

    def block(ref, index):
        return ref.at[pl.ds(pl.multiple_of(index * each, each), each), :]

    def send_column(to_x, to_y, same_chip=False):
        for e in range(1 if same_chip else 0, chans):
            to_chan = chan if e == 0 else 1 - chan
            to = (to_x * side + to_y) * chans + to_chan
            send(block(spectrum, to), block(columns, me), send_b, recv_b, place(to_x, to_y, to_chan))

    middle_way = side // 2
    send_column(ahead(x, middle_way), ahead(y, middle_way))
    send_column(ahead(x, middle_way), y)
    send_column(x, ahead(y, middle_way))

    @pl.loop(1, middle_way * middle_way)
    def _(k):
        a, b = middle_way - k // middle_way, k % middle_way
        send_column(ahead(x, a), ahead(y, b))
        send_column(behind(x, b), ahead(y, a))
        send_column(behind(x, a), behind(y, b))
        send_column(ahead(x, b), behind(y, a))

    send_column(x, y, same_chip=True)

    own = pl.ds(pl.multiple_of(me * each, each), each)
    columns[own, :] = spectrum[own, :]
    for k in (8, 9, 10):
        loads[k].wait()
    await_bytes(columns.at[pl.ds(0, (count - 1) * each), :], recv_b)

    wide = G // ROWS
    for lane in range(groups):
        real = columns[pl.ds(lane, count, stride=each), :]
        imag = columns[pl.ds(groups + lane, count, stride=each), :]
        first = table_dot(col_table, jnp.concatenate([real, imag], axis=0), 0)
        re, im = first[:wide], first[wide:]
        c, s = col_twist[0], col_twist[1]
        turned = jnp.concatenate([re * c - im * s, re * s + im * c], axis=1)
        last = table_dot(last_table, turned, 1)
        tall = LANES // ROWS
        for l2 in range(ROWS):
            out[tall * lane : tall * (lane + 1), wide * l2 : wide * (l2 + 1)] = last[tall * l2 : tall * (l2 + 1)]

    await_bytes(packed.at[pl.ds(0, (line - 1) * side)], send_1)
    await_bytes(landed.at[pl.ds(0, side - 1)], send_2)
    await_bytes(rows.at[pl.ds(0, BLOCKS - strip)], send_x)
    await_bytes(columns.at[pl.ds(0, (count - 1) * each), :], send_b)


def body(*inputs):
    tiles, chans = lax.axis_size("tile"), lax.axis_size("chan")
    count, side = tiles * chans, math.isqrt(tiles)
    operands = [*inputs, *(jnp.asarray(table) for table in tables(count))]
    return pl.pallas_call(
        functools.partial(kernel, tiles, chans),
        out_shape=jax.ShapeDtypeStruct((OUT_ROWS, G), F32),
        in_specs=[pl.BlockSpec(memory_space=pl.ANY)] * len(operands),
        out_specs=pl.BlockSpec(memory_space=pltpu.VMEM),
        scratch_shapes=[pltpu.VMEM(operand.shape, operand.dtype) for operand in operands]
        + [
            pltpu.VMEM((3, NT, NT * CAP), F32),
            pltpu.VMEM((count, 3, LANES), F32),
            pltpu.VMEM((side, side * chans, 3, LANES), F32),
            pltpu.VMEM((side, side * chans, 3, LANES), F32),
            pltpu.VMEM((3, LANES, count), F32),
            pltpu.VMEM((BLOCKS // QUARTERS, TILE, LANES), F32),
            pltpu.VMEM((BLOCKS, ROWS, LANES), F32),
            pltpu.VMEM((BLOCKS * ROWS, 2 * LANES), BF16),
            pltpu.VMEM((BLOCKS * ROWS, 2 * LANES), BF16),
            pltpu.VMEM((count * 8, LANES), F32),
            pltpu.VMEM((count * 8, LANES), F32),
            pltpu.SemaphoreType.DMA((len(operands),)),
        ]
        + [pltpu.SemaphoreType.DMA] * 8,
        compiler_params=pltpu.CompilerParams(collective_id=0, has_side_effects=True),
    )(*operands)


def solution(mesh):
    spec = P(("layout", "tile", "chan"), None, None)
    return jax.shard_map(
        body,
        mesh=mesh,
        in_specs=(spec,) * 5,
        out_specs=P(("layout", "tile", "chan"), None),
        check_vma=False,
    )
```

```python
import functools
import math

import jax
import jax.numpy as jnp
import numpy as np
from jax import lax
from jax.experimental import pallas as pl
from jax.experimental.pallas import tpu as pltpu
from jax.sharding import PartitionSpec as P

G = 4096
TILE = 64
CAP = 4
NT = 64
LANES = 128
QUARTERS = 4
ROWS = TILE // QUARTERS
BLOCKS = G // LANES
OUT_ROWS = 32
MESH = pl.DeviceIdType.MESH
F32 = jnp.float32
BF16 = jnp.bfloat16


def two_parts(table):
    table = np.asarray(table, np.float32)
    high = table.astype(BF16)
    low = (table - high.astype(np.float32)).astype(BF16)
    return np.concatenate([high, low], axis=0)


@functools.lru_cache
def tables(devices):
    spread = (np.arange(NT)[:, None] == np.arange(NT * CAP)[None, :] // CAP).astype(BF16)
    turn = 2.0 * np.pi * np.outer(np.arange(LANES), np.arange(LANES)) / LANES
    cos, sin = np.cos(turn), np.sin(turn)
    row_table = two_parts(np.block([[cos, -sin], [sin, cos]]))
    turn = 2.0 * np.pi * np.outer(np.arange(BLOCKS), np.arange(LANES)) / G
    row_twist = np.stack([np.cos(turn), np.sin(turn)]).astype(np.float32)
    wide = G // ROWS
    turn = 2.0 * np.pi * np.outer(np.arange(wide), np.arange(devices)) / wide
    cos, sin = np.cos(turn), np.sin(turn)
    col_table = two_parts(np.block([[cos, -sin], [sin, cos]]))
    turn = 2.0 * np.pi * np.outer(np.arange(wide), np.arange(LANES) % ROWS) / G
    col_twist = np.stack([np.cos(turn), np.sin(turn)]).astype(np.float32)
    group = LANES // ROWS
    out_index = np.arange(ROWS * group)
    lane = np.arange(LANES)
    same = (out_index[:, None] % group == lane[None, :] // ROWS) / math.sqrt(devices * NT * NT * CAP)
    turn = 2.0 * np.pi * np.outer(out_index // group, lane % ROWS) / ROWS
    last_table = two_parts(np.concatenate([same * np.cos(turn), -same * np.sin(turn)], axis=1))
    return spread, row_table, row_twist, col_table, col_twist, last_table


def split(value):
    high = value.astype(BF16)
    return high, (value - high.astype(F32)).astype(BF16)


def dot(left, right, right_dim):
    return lax.dot_general(left, right, (((1,), (right_dim,)), ((), ())), preferred_element_type=F32)


def table_dot(table, value, right_dim):
    high, low = split(value)
    half = table.shape[0] // 2
    both = dot(table[...], high, right_dim)
    return both[:half] + both[half:] + dot(table[:half], low, right_dim)


def times(value, real, imag):
    v_re, v_im = value
    if abs(imag) < 1e-12:
        if abs(real - 1.0) < 1e-12:
            return value
        return v_re * real, None if v_im is None else v_im * real
    if v_im is None:
        return (None if abs(real) < 1e-12 else v_re * real), v_re * imag
    if abs(real) < 1e-12:
        return -v_im * imag, v_re * imag
    return v_re * real - v_im * imag, v_re * imag + v_im * real


def plus(a, b, sign):
    if b is None:
        return a
    if a is None:
        return b if sign > 0 else -b
    return a + b if sign > 0 else a - b


def real_transform(values):
    count = len(values)
    if count == 1:
        return [(values[0], None)]
    if count == 2:
        return [(values[0] + values[1], None), (values[0] - values[1], None)]
    even, odd = real_transform(values[0::2]), real_transform(values[1::2])
    out = [None] * (count // 2 + 1)
    for k in range(count // 4 + 1):
        turn = 2.0 * math.pi * k / count
        turned = times(odd[k], math.cos(turn), math.sin(turn))
        out[k] = (plus(even[k][0], turned[0], 1), plus(even[k][1], turned[1], 1))
        far_im = plus(even[k][1], turned[1], -1)
        out[count // 2 - k] = (plus(even[k][0], turned[0], -1), None if far_im is None else -far_im)
    return out


def kernel(tiles, chans, *refs):
    inputs, tables_in, refs = refs[:5], refs[5:11], refs[11:]
    out, refs = refs[0], refs[1:]
    weight, frac_u, frac_v, code, fill = refs[:5]
    spread, row_table, row_twist, col_table, col_twist, last_table = refs[5:11]
    sample, packed, middle, landed, sorted_, slab, rows, high, low, spectrum, columns = refs[11:22]
    load, send_1, recv_1, send_2, recv_2, send_x, recv_x, send_b, recv_b = refs[22:]
    side = math.isqrt(tiles)
    count = tiles * chans
    layout, tile, chan = lax.axis_index("layout"), lax.axis_index("tile"), lax.axis_index("chan")
    x, y = lax.div(tile, side), lax.rem(tile, side)
    along, across = jnp.where(chan == 0, x, y), jnp.where(chan == 0, y, x)
    me = tile * chans + chan
    mine = lax.rem(me, QUARTERS)
    far_first = sorted(range(side), key=lambda d: -min(d, side - d))

    def ahead(value, step):
        value = value + step
        return jnp.where(value >= side, value - side, value)

    def behind(value, step):
        value = value - step
        return jnp.where(value < 0, value + side, value)

    def place(to_x, to_y, to_chan):
        return (layout, to_x * side + to_y, to_chan)

    def turned_place(to_along, to_across, to_chan):
        return place(
            jnp.where(chan == 0, to_along, to_across), jnp.where(chan == 0, to_across, to_along), to_chan
        )

    def send(src, dst, send_sem, recv_sem, device):
        pltpu.make_async_remote_copy(
            src_ref=src,
            dst_ref=dst,
            send_sem=send_sem,
            recv_sem=recv_sem,
            device_id=device,
            device_id_type=MESH,
        ).start()

    def await_bytes(ref, sem):
        pltpu.make_async_copy(ref, ref, sem).wait()

    steps = [d for d in far_first if d != 0]
    barrier = pltpu.get_barrier_semaphore()
    senders = [turned_place(ahead(along, d), across, e) for d in steps for e in range(chans)]
    senders += [turned_place(along, ahead(across, d), chan) for d in steps]
    senders += [place(x, y, 1 - chan)]
    for device in senders:
        pl.semaphore_signal(barrier, inc=1, device_id=device, device_id_type=MESH)

    loads = [
        pltpu.make_async_copy(src, dst, load.at[k])
        for k, (src, dst) in enumerate(zip([*inputs, *tables_in], refs[:11], strict=True))
    ]
    for k in (4, 5, 0, 3, 1, 2, 6, 7, 8, 9, 10):
        loads[k].start()
    for k in range(6):
        loads[k].wait()

    fill_wide = dot(fill[0].astype(F32).astype(BF16), spread[...], 0)
    slot = lax.broadcasted_iota(jnp.int32, (NT, NT * CAP), 1) % CAP
    sample[0] = jnp.where(slot.astype(F32) < fill_wide, weight[0], 0.0)
    far = lax.broadcasted_iota(jnp.int32, (NT, NT * CAP), 0) >= NT // 2
    for part, position in (
        (1, (code[0] >> 6).astype(F32) + frac_u[0]),
        (2, (code[0] & (TILE - 1)).astype(F32) + frac_v[0]),
    ):
        sample[part] = jnp.where(far, TILE - position, position) * 0.25

    lower = lax.broadcasted_iota(jnp.int32, (1, LANES), 1) < LANES // 2

    @pl.loop(0, side)
    def _(to_x):
        for near_y in range(side // 2):
            p = to_x * (side // 2) + near_y
            for part in range(3):
                near = sample[part, pl.ds(p, 1), :]
                away = sample[part, pl.ds(NT - 1 - p, 1), :]
                for q in range(QUARTERS):
                    a = near[:, (q // 2) * LANES : (q // 2 + 1) * LANES]
                    b = away[:, (1 - q // 2) * LANES : (2 - q // 2) * LANES]
                    if q % 2 == 0:
                        row = jnp.where(lower, a, b)
                    else:
                        row = pltpu.roll(jnp.where(lower, b, a), LANES // 2, 1)
                    to_y, to_chan = 2 * near_y + q // 2, q % 2
                    where = to_x * side + to_y if to_chan == 0 else tiles + to_y * side + to_x
                    packed[where, pl.ds(part, 1), :] = row

    pl.semaphore_wait(barrier, len(senders))

    def strand(start):
        return packed.at[pl.ds(start * side, side)]

    for d in steps:
        to_x, to_y = ahead(x, d), ahead(y, d)
        send(strand(to_x), middle.at[:, x * chans + chan], send_1, recv_1, place(to_x, y, 0))
        send(strand(side + to_y), middle.at[:, y * chans + chan], send_1, recv_1, place(x, to_y, 1))
    send(
        strand(jnp.where(chan == 0, side + y, x)),
        middle.at[:, across * chans + chan],
        send_1,
        recv_1,
        place(x, y, 1 - chan),
    )
    middle[:, along * chans + chan] = packed[pl.ds((chan * side + along) * side, side)]
    await_bytes(packed.at[pl.ds(0, (2 * side - 1) * side)], recv_1)
    for d in steps:
        to = ahead(across, d)
        send(middle.at[to], landed.at[across], send_2, recv_2, turned_place(along, to, chan))
    landed[across] = middle[across]
    await_bytes(landed.at[pl.ds(0, side - 1)], recv_2)

    for part in range(3):
        sorted_[part] = landed[:, :, part, :].reshape(count, LANES).T

    cell = lax.broadcasted_iota(jnp.int32, (TILE, count), 0).astype(F32) * 0.25

    def taper(row, where):
        scaled = cell - row[where]
        inner = jnp.maximum(1.0 - scaled * scaled, 0.0)
        return inner * inner

    def one_tile(k):
        total = jnp.zeros((2 * TILE, 2 * TILE), F32)
        starts = [CAP * k, NT * CAP // 2 - CAP - CAP * k]
        for start in starts:
            for pair in range(CAP // 2):
                lefts, rights = [], []
                for slot in range(2):
                    where = pl.ds(start + 2 * pair + slot, 1)
                    u_high, u_low = split(taper(sorted_.at[1], where) * sorted_[0, where])
                    v_high, v_low = split(taper(sorted_.at[2], where))
                    lefts.append(jnp.concatenate([u_high, u_low], axis=0))
                    rights.append(jnp.concatenate([v_high, v_low], axis=0))
                total += dot(jnp.concatenate(lefts, axis=1), jnp.concatenate(rights, axis=1), 1)
        return total[:TILE] + total[TILE:]

    upper_half = lax.broadcasted_iota(jnp.int32, (TILE, LANES), 1) >= TILE
    strip = BLOCKS // QUARTERS
    others = []
    for hop in range(1, QUARTERS):
        other = lax.rem(mine + hop, QUARTERS)
        index = me - mine + other
        others.append((other, (layout, lax.div(index, chans), lax.rem(index, chans))))

    def row_range(index):
        return pl.ds(pl.multiple_of(index * ROWS, ROWS), ROWS)

    @pl.loop(0, strip)
    def _(pair):
        first, second = one_tile(2 * pair), one_tile(2 * pair + 1)
        first = first + pltpu.roll(first, TILE, 1)
        second = second + pltpu.roll(second, TILE, 1)
        slab[pair] = jnp.where(upper_half, second, first)
        for other, device in others:
            send(slab.at[pair, row_range(other), :], rows.at[mine * strip + pair], send_x, recv_x, device)

    rows[pl.ds(mine * strip, strip)] = slab[:, row_range(mine), :]
    for k in (6, 7):
        loads[k].wait()
    await_bytes(rows.at[pl.ds(0, BLOCKS - strip)], recv_x)

    waves = real_transform([rows[t] for t in range(BLOCKS)])
    for k in range(BLOCKS):
        re, im = waves[min(k, BLOCKS - k)]
        c, s = row_twist[0, k : k + 1, :], row_twist[1, k : k + 1, :]
        if im is None:
            turned = (re * c, re * s)
        elif k <= BLOCKS // 2:
            turned = (re * c - im * s, re * s + im * c)
        else:
            turned = (re * c + im * s, re * s - im * c)
        for part in range(2):
            upper, rest = split(turned[part])
            high[ROWS * k : ROWS * (k + 1), LANES * part : LANES * (part + 1)] = upper
            low[ROWS * k : ROWS * (k + 1), LANES * part : LANES * (part + 1)] = rest
    groups = BLOCKS * ROWS // LANES
    for lane in range(0, groups, 2):
        where = slice(LANES * lane, LANES * (lane + 2))
        both = dot(row_table[...], high[where], 1)
        half = 2 * LANES
        both = both[:half] + both[half:] + dot(row_table[:half], low[where], 1)
        for part in range(2):
            for extra in range(2):
                spectrum[pl.ds(part * groups + lane + extra, count, stride=2 * groups), :] = both[
                    part * LANES : (part + 1) * LANES, extra * LANES : (extra + 1) * LANES
                ]

    each = 2 * groups

    def block(ref, index):
        return ref.at[pl.ds(pl.multiple_of(index * each, each), each), :]

    def send_column(to_x, to_y, same_chip=False):
        for e in range(1 if same_chip else 0, chans):
            to_chan = chan if e == 0 else 1 - chan
            to = (to_x * side + to_y) * chans + to_chan
            send(block(spectrum, to), block(columns, me), send_b, recv_b, place(to_x, to_y, to_chan))

    middle_way = side // 2
    send_column(ahead(x, middle_way), ahead(y, middle_way))
    send_column(ahead(x, middle_way), y)
    send_column(x, ahead(y, middle_way))

    @pl.loop(1, middle_way * middle_way)
    def _(k):
        a, b = middle_way - k // middle_way, k % middle_way
        send_column(ahead(x, a), ahead(y, b))
        send_column(behind(x, b), ahead(y, a))
        send_column(behind(x, a), behind(y, b))
        send_column(ahead(x, b), behind(y, a))

    send_column(x, y, same_chip=True)

    own = pl.ds(pl.multiple_of(me * each, each), each)
    columns[own, :] = spectrum[own, :]
    for k in (8, 9, 10):
        loads[k].wait()
    await_bytes(columns.at[pl.ds(0, (count - 1) * each), :], recv_b)

    wide = G // ROWS
    for lane in range(groups):
        real = columns[pl.ds(lane, count, stride=each), :]
        imag = columns[pl.ds(groups + lane, count, stride=each), :]
        first = table_dot(col_table, jnp.concatenate([real, imag], axis=0), 0)
        re, im = first[:wide], first[wide:]
        c, s = col_twist[0], col_twist[1]
        turned = jnp.concatenate([re * c - im * s, re * s + im * c], axis=1)
        last = table_dot(last_table, turned, 1)
        tall = LANES // ROWS
        for l2 in range(ROWS):
            out[tall * lane : tall * (lane + 1), wide * l2 : wide * (l2 + 1)] = last[tall * l2 : tall * (l2 + 1)]

    await_bytes(packed.at[pl.ds(0, (2 * side - 1) * side)], send_1)
    await_bytes(landed.at[pl.ds(0, side - 1)], send_2)
    await_bytes(rows.at[pl.ds(0, BLOCKS - strip)], send_x)
    await_bytes(columns.at[pl.ds(0, (count - 1) * each), :], send_b)


def body(*inputs):
    tiles, chans = lax.axis_size("tile"), lax.axis_size("chan")
    count, side = tiles * chans, math.isqrt(tiles)
    operands = [*inputs, *(jnp.asarray(table) for table in tables(count))]
    return pl.pallas_call(
        functools.partial(kernel, tiles, chans),
        out_shape=jax.ShapeDtypeStruct((OUT_ROWS, G), F32),
        in_specs=[pl.BlockSpec(memory_space=pl.ANY)] * len(operands),
        out_specs=pl.BlockSpec(memory_space=pltpu.VMEM),
        scratch_shapes=[pltpu.VMEM(operand.shape, operand.dtype) for operand in operands]
        + [
            pltpu.VMEM((3, NT, NT * CAP), F32),
            pltpu.VMEM((count, 3, LANES), F32),
            pltpu.VMEM((side, side * chans, 3, LANES), F32),
            pltpu.VMEM((side, side * chans, 3, LANES), F32),
            pltpu.VMEM((3, LANES, count), F32),
            pltpu.VMEM((BLOCKS // QUARTERS, TILE, LANES), F32),
            pltpu.VMEM((BLOCKS, ROWS, LANES), F32),
            pltpu.VMEM((BLOCKS * ROWS, 2 * LANES), BF16),
            pltpu.VMEM((BLOCKS * ROWS, 2 * LANES), BF16),
            pltpu.VMEM((count * 8, LANES), F32),
            pltpu.VMEM((count * 8, LANES), F32),
            pltpu.SemaphoreType.DMA((len(operands),)),
        ]
        + [pltpu.SemaphoreType.DMA] * 8,
        compiler_params=pltpu.CompilerParams(collective_id=0, has_side_effects=True),
    )(*operands)


def solution(mesh):
    spec = P(("layout", "tile", "chan"), None, None)
    return jax.shard_map(
        body,
        mesh=mesh,
        in_specs=(spec,) * 5,
        out_specs=P(("layout", "tile", "chan"), None),
        check_vma=False,
    )
```

```python
import functools
import math

import jax
import jax.numpy as jnp
import numpy as np
from jax import lax
from jax.experimental import pallas as pl
from jax.experimental.pallas import tpu as pltpu
from jax.sharding import PartitionSpec as P

G = 4096
TILE = 64
CAP = 4
NT = 64
LANES = 128
QUARTERS = 4
ROWS = TILE // QUARTERS
BLOCKS = G // LANES
OUT_ROWS = 32
MESH = pl.DeviceIdType.MESH
VMEM_LIMIT = 16 * 2**20
F32 = jnp.float32
BF16 = jnp.bfloat16


def two_parts(table):
    table = np.asarray(table, np.float32)
    high = table.astype(BF16)
    low = (table - high.astype(np.float32)).astype(BF16)
    return np.concatenate([high, low], axis=0)


@functools.lru_cache
def tables(devices):
    spread = (np.arange(NT)[:, None] == np.arange(NT * CAP)[None, :] // CAP).astype(BF16)
    turn = 2.0 * np.pi * np.outer(np.arange(LANES), np.arange(LANES)) / LANES
    cos, sin = np.cos(turn), np.sin(turn)
    row_table = two_parts(np.block([[cos, -sin], [sin, cos]]))
    turn = 2.0 * np.pi * np.outer(np.arange(BLOCKS), np.arange(LANES)) / G
    row_twist = np.stack([np.cos(turn), np.sin(turn)]).astype(np.float32)
    wide = G // ROWS
    turn = 2.0 * np.pi * np.outer(np.arange(wide), np.arange(devices)) / wide
    cos, sin = np.cos(turn), np.sin(turn)
    col_table = two_parts(np.block([[cos, -sin], [sin, cos]]))
    turn = 2.0 * np.pi * np.outer(np.arange(wide), np.arange(LANES) % ROWS) / G
    col_twist = np.stack([np.cos(turn), np.sin(turn)]).astype(np.float32)
    group = LANES // ROWS
    out_index = np.arange(ROWS * group)
    lane = np.arange(LANES)
    same = (out_index[:, None] % group == lane[None, :] // ROWS) / math.sqrt(devices * NT * NT * CAP)
    turn = 2.0 * np.pi * np.outer(out_index // group, lane % ROWS) / ROWS
    last_table = two_parts(np.concatenate([same * np.cos(turn), -same * np.sin(turn)], axis=1))
    return spread, row_table, row_twist, col_table, col_twist, last_table


def split(value):
    high = value.astype(BF16)
    return high, (value - high.astype(F32)).astype(BF16)


def dot(left, right, right_dim):
    return lax.dot_general(left, right, (((1,), (right_dim,)), ((), ())), preferred_element_type=F32)


def table_dot(table, value, right_dim):
    high, low = split(value)
    half = table.shape[0] // 2
    both = dot(table[...], high, right_dim)
    return both[:half] + both[half:] + dot(table[:half], low, right_dim)


def times(value, real, imag):
    v_re, v_im = value
    if abs(imag) < 1e-12:
        if abs(real - 1.0) < 1e-12:
            return value
        return v_re * real, None if v_im is None else v_im * real
    if v_im is None:
        return (None if abs(real) < 1e-12 else v_re * real), v_re * imag
    if abs(real) < 1e-12:
        return -v_im * imag, v_re * imag
    return v_re * real - v_im * imag, v_re * imag + v_im * real


def plus(a, b, sign):
    if b is None:
        return a
    if a is None:
        return b if sign > 0 else -b
    return a + b if sign > 0 else a - b


def real_transform(values):
    count = len(values)
    if count == 1:
        return [(values[0], None)]
    if count == 2:
        return [(values[0] + values[1], None), (values[0] - values[1], None)]
    even, odd = real_transform(values[0::2]), real_transform(values[1::2])
    out = [None] * (count // 2 + 1)
    for k in range(count // 4 + 1):
        turn = 2.0 * math.pi * k / count
        turned = times(odd[k], math.cos(turn), math.sin(turn))
        out[k] = (plus(even[k][0], turned[0], 1), plus(even[k][1], turned[1], 1))
        far_im = plus(even[k][1], turned[1], -1)
        out[count // 2 - k] = (plus(even[k][0], turned[0], -1), None if far_im is None else -far_im)
    return out


def far_chips_first(side):
    half = side // 2
    ties = [step for j in range(side) for step in ([(half, j), (j, half)] if j != half else [(half, half)])]
    quarter = [(a, b) for a in range(half - 1, 0, -1) for b in range(half - 1, -1, -1)]
    quarter.sort(key=lambda step: -sum(step))
    turned = [step for a, b in quarter for step in ((a, b), (-b, a), (-a, -b), (b, -a))]
    return [(dx % side, dy % side) for dx, dy in ties + turned]


def kernel(tiles, chans, *refs):
    operands, columns, refs = refs[:8], refs[8], refs[9:]
    weight, frac_u, frac_v, code, fill, spread, row_table, row_twist = refs[:8]
    sample, packed, middle, landed, sorted_, slab, rows, high, low, spectrum = refs[8:18]
    load, send_1, recv_1, send_2, recv_2, send_x, recv_x, send_b, recv_b = refs[18:]
    side = math.isqrt(tiles)
    count = tiles * chans
    layout, tile, chan = lax.axis_index("layout"), lax.axis_index("tile"), lax.axis_index("chan")
    x, y = lax.div(tile, side), lax.rem(tile, side)
    along, across = jnp.where(chan == 0, x, y), jnp.where(chan == 0, y, x)
    me = tile * chans + chan
    mine = lax.rem(me, QUARTERS)
    far_first = sorted(range(side), key=lambda d: -min(d, side - d))

    def ahead(value, step):
        if step == 0:
            return value
        value = value + step
        return jnp.where(value >= side, value - side, value)

    def place(to_x, to_y, to_chan):
        return (layout, to_x * side + to_y, to_chan)

    def turned_place(to_along, to_across, to_chan):
        return place(
            jnp.where(chan == 0, to_along, to_across), jnp.where(chan == 0, to_across, to_along), to_chan
        )

    def send(src, dst, send_sem, recv_sem, device):
        pltpu.make_async_remote_copy(
            src_ref=src,
            dst_ref=dst,
            send_sem=send_sem,
            recv_sem=recv_sem,
            device_id=device,
            device_id_type=MESH,
        ).start()

    def await_bytes(ref, sem):
        pltpu.make_async_copy(ref, ref, sem).wait()

    steps = [d for d in far_first if d != 0]
    barrier = pltpu.get_barrier_semaphore()
    senders = [turned_place(ahead(along, d), across, e) for d in steps for e in range(chans)]
    senders += [turned_place(along, ahead(across, d), chan) for d in steps]
    senders += [place(x, y, 1 - chan)]
    for device in senders:
        pl.semaphore_signal(barrier, inc=1, device_id=device, device_id_type=MESH)

    loads = [
        pltpu.make_async_copy(src, dst, load.at[k])
        for k, (src, dst) in enumerate(zip(operands, refs[:8], strict=True))
    ]
    for k in (4, 5, 0, 3, 1, 2, 6, 7):
        loads[k].start()
    for k in range(6):
        loads[k].wait()

    fill_wide = dot(fill[0].astype(F32).astype(BF16), spread[...], 0)
    slot = lax.broadcasted_iota(jnp.int32, (NT, NT * CAP), 1) % CAP
    sample[0] = jnp.where(slot.astype(F32) < fill_wide, weight[0], 0.0)
    far = lax.broadcasted_iota(jnp.int32, (NT, NT * CAP), 0) >= NT // 2
    for part, position in (
        (1, (code[0] >> 6).astype(F32) + frac_u[0]),
        (2, (code[0] & (TILE - 1)).astype(F32) + frac_v[0]),
    ):
        sample[part] = jnp.where(far, TILE - position, position) * 0.25

    lower = lax.broadcasted_iota(jnp.int32, (1, LANES), 1) < LANES // 2

    @pl.loop(0, side)
    def _(to_x):
        for near_y in range(side // 2):
            p = to_x * (side // 2) + near_y
            for part in range(3):
                near = sample[part, pl.ds(p, 1), :]
                away = sample[part, pl.ds(NT - 1 - p, 1), :]
                for q in range(QUARTERS):
                    a = near[:, (q // 2) * LANES : (q // 2 + 1) * LANES]
                    b = away[:, (1 - q // 2) * LANES : (2 - q // 2) * LANES]
                    if q % 2 == 0:
                        row = jnp.where(lower, a, b)
                    else:
                        row = pltpu.roll(jnp.where(lower, b, a), LANES // 2, 1)
                    to_y, to_chan = 2 * near_y + q // 2, q % 2
                    where = to_x * side + to_y if to_chan == 0 else tiles + to_y * side + to_x
                    packed[where, pl.ds(part, 1), :] = row

    pl.semaphore_wait(barrier, len(senders))

    def strand(start):
        return packed.at[pl.ds(start * side, side)]

    for d in steps:
        to_x, to_y = ahead(x, d), ahead(y, d)
        send(strand(to_x), middle.at[:, x * chans + chan], send_1, recv_1, place(to_x, y, 0))
        send(strand(side + to_y), middle.at[:, y * chans + chan], send_1, recv_1, place(x, to_y, 1))
    send(
        strand(jnp.where(chan == 0, side + y, x)),
        middle.at[:, across * chans + chan],
        send_1,
        recv_1,
        place(x, y, 1 - chan),
    )
    middle[:, along * chans + chan] = packed[pl.ds((chan * side + along) * side, side)]
    await_bytes(packed.at[pl.ds(0, (2 * side - 1) * side)], recv_1)
    for d in steps:
        to = ahead(across, d)
        send(middle.at[to], landed.at[across], send_2, recv_2, turned_place(along, to, chan))
    landed[across] = middle[across]
    await_bytes(landed.at[pl.ds(0, side - 1)], recv_2)

    for part in range(3):
        sorted_[part] = landed[:, :, part, :].reshape(count, LANES).T

    cell = lax.broadcasted_iota(jnp.int32, (TILE, count), 0).astype(F32) * 0.25

    def taper(row, where):
        scaled = cell - row[where]
        inner = jnp.maximum(1.0 - scaled * scaled, 0.0)
        return inner * inner

    def one_tile(k):
        total = jnp.zeros((2 * TILE, 2 * TILE), F32)
        starts = [CAP * k, NT * CAP // 2 - CAP - CAP * k]
        for start in starts:
            for pair in range(CAP // 2):
                lefts, rights = [], []
                for slot in range(2):
                    where = pl.ds(start + 2 * pair + slot, 1)
                    u_high, u_low = split(taper(sorted_.at[1], where) * sorted_[0, where])
                    v_high, v_low = split(taper(sorted_.at[2], where))
                    lefts.append(jnp.concatenate([u_high, u_low], axis=0))
                    rights.append(jnp.concatenate([v_high, v_low], axis=0))
                total += dot(jnp.concatenate(lefts, axis=1), jnp.concatenate(rights, axis=1), 1)
        return total[:TILE] + total[TILE:]

    upper_half = lax.broadcasted_iota(jnp.int32, (TILE, LANES), 1) >= TILE
    strip = BLOCKS // QUARTERS
    others = []
    for hop in range(1, QUARTERS):
        other = lax.rem(mine + hop, QUARTERS)
        index = me - mine + other
        others.append((other, (layout, lax.div(index, chans), lax.rem(index, chans))))

    def row_range(index):
        return pl.ds(pl.multiple_of(index * ROWS, ROWS), ROWS)

    @pl.loop(0, strip)
    def _(pair):
        first, second = one_tile(2 * pair), one_tile(2 * pair + 1)
        first = first + pltpu.roll(first, TILE, 1)
        second = second + pltpu.roll(second, TILE, 1)
        slab[pair] = jnp.where(upper_half, second, first)
        for other, device in others:
            send(slab.at[pair, row_range(other), :], rows.at[mine * strip + pair], send_x, recv_x, device)

    rows[pl.ds(mine * strip, strip)] = slab[:, row_range(mine), :]
    for k in (6, 7):
        loads[k].wait()
    await_bytes(rows.at[pl.ds(0, BLOCKS - strip)], recv_x)

    waves = real_transform([rows[t] for t in range(BLOCKS)])
    for k in range(BLOCKS):
        re, im = waves[min(k, BLOCKS - k)]
        c, s = row_twist[0, k : k + 1, :], row_twist[1, k : k + 1, :]
        if im is None:
            turned = (re * c, re * s)
        elif k <= BLOCKS // 2:
            turned = (re * c - im * s, re * s + im * c)
        else:
            turned = (re * c + im * s, re * s - im * c)
        for part in range(2):
            upper, rest = split(turned[part])
            high[ROWS * k : ROWS * (k + 1), LANES * part : LANES * (part + 1)] = upper
            low[ROWS * k : ROWS * (k + 1), LANES * part : LANES * (part + 1)] = rest
    groups = BLOCKS * ROWS // LANES
    for lane in range(0, groups, 2):
        where = slice(LANES * lane, LANES * (lane + 2))
        both = dot(row_table[...], high[where], 1)
        half = 2 * LANES
        both = both[:half] + both[half:] + dot(row_table[:half], low[where], 1)
        for part in range(2):
            for extra in range(2):
                spectrum[pl.ds(part * groups + lane + extra, count, stride=2 * groups), :] = both[
                    part * LANES : (part + 1) * LANES, extra * LANES : (extra + 1) * LANES
                ]

    each = 2 * groups

    def block(ref, index):
        return ref.at[pl.ds(pl.multiple_of(index * each, each), each), :]

    def send_column(to_x, to_y, same_chip=False):
        for e in range(1 if same_chip else 0, chans):
            to_chan = chan if e == 0 else 1 - chan
            to = (to_x * side + to_y) * chans + to_chan
            send(block(spectrum, to), block(columns, me), send_b, recv_b, place(to_x, to_y, to_chan))

    for dx, dy in far_chips_first(side):
        send_column(ahead(x, dx), ahead(y, dy))
    send_column(x, y, same_chip=True)

    own = pltpu.make_async_copy(block(spectrum, me), block(columns, me), load.at[0])
    own.start()
    own.wait()
    await_bytes(columns.at[pl.ds(0, (count - 1) * each), :], recv_b)
    await_bytes(packed.at[pl.ds(0, (2 * side - 1) * side)], send_1)
    await_bytes(landed.at[pl.ds(0, side - 1)], send_2)
    await_bytes(rows.at[pl.ds(0, BLOCKS - strip)], send_x)
    await_bytes(columns.at[pl.ds(0, (count - 1) * each), :], send_b)


def column_kernel(columns, col_table, col_twist, last_table, out, image, sem):
    count = col_table.shape[1] // 2
    each = columns.shape[0] // count
    groups, wide, tall = each // 2, G // ROWS, LANES // ROWS
    stores = []
    for pair in range(0, groups, 2):
        parts = [
            [columns[pl.ds(part * groups + pair + extra, count, stride=each), :] for part in range(2)]
            for extra in range(2)
        ]
        stacked = jnp.concatenate([jnp.concatenate(part, axis=0) for part in parts], axis=1)
        first = table_dot(col_table, stacked, 0)
        c, s = col_twist[0], col_twist[1]
        for extra in range(2):
            lane = pair + extra
            re = first[:wide, extra * LANES : (extra + 1) * LANES]
            im = first[wide:, extra * LANES : (extra + 1) * LANES]
            turned = jnp.concatenate([re * c - im * s, re * s + im * c], axis=1)
            last = table_dot(last_table, turned, 1)
            for l2 in range(ROWS):
                image[tall * lane : tall * (lane + 1), wide * l2 : wide * (l2 + 1)] = last[tall * l2 : tall * (l2 + 1)]
            here = pl.ds(tall * lane, tall)
            stores.append(pltpu.make_async_copy(image.at[here, :], out.at[here, :], sem.at[lane]))
            stores[-1].start()
    for store in stores:
        store.wait()


def body(*inputs):
    tiles, chans = lax.axis_size("tile"), lax.axis_size("chan")
    count, side = tiles * chans, math.isqrt(tiles)
    constants = [jnp.asarray(table) for table in tables(count)]
    operands = [pltpu.with_memory_space_constraint(v, pltpu.HBM) for v in [*inputs, *constants[:3]]]
    columns = pl.pallas_call(
        functools.partial(kernel, tiles, chans),
        out_shape=jax.ShapeDtypeStruct((count * 8, LANES), F32),
        in_specs=[pl.BlockSpec(memory_space=pltpu.HBM)] * len(operands),
        out_specs=pl.BlockSpec(memory_space=pl.ANY),
        scratch_shapes=[pltpu.VMEM(operand.shape, operand.dtype) for operand in operands]
        + [
            pltpu.VMEM((3, NT, NT * CAP), F32),
            pltpu.VMEM((count, 3, LANES), F32),
            pltpu.VMEM((side, side * chans, 3, LANES), F32),
            pltpu.VMEM((side, side * chans, 3, LANES), F32),
            pltpu.VMEM((3, LANES, count), F32),
            pltpu.VMEM((BLOCKS // QUARTERS, TILE, LANES), F32),
            pltpu.VMEM((BLOCKS, ROWS, LANES), F32),
            pltpu.VMEM((BLOCKS * ROWS, 2 * LANES), BF16),
            pltpu.VMEM((BLOCKS * ROWS, 2 * LANES), BF16),
            pltpu.VMEM((count * 8, LANES), F32),
            pltpu.SemaphoreType.DMA((len(operands),)),
        ]
        + [pltpu.SemaphoreType.DMA] * 8,
        compiler_params=pltpu.CompilerParams(
            collective_id=0, has_side_effects=True, vmem_limit_bytes=VMEM_LIMIT
        ),
    )(*operands)
    return pl.pallas_call(
        column_kernel,
        out_shape=jax.ShapeDtypeStruct((OUT_ROWS, G), F32),
        in_specs=[pl.BlockSpec(memory_space=pltpu.VMEM)] * 4,
        out_specs=pl.BlockSpec(memory_space=pl.ANY),
        scratch_shapes=[
            pltpu.VMEM((OUT_ROWS, G), F32),
            pltpu.SemaphoreType.DMA((BLOCKS * ROWS // LANES,)),
        ],
        compiler_params=pltpu.CompilerParams(vmem_limit_bytes=VMEM_LIMIT),
    )(columns, *constants[3:])


def solution(mesh):
    spec = P(("layout", "tile", "chan"), None, None)
    return jax.shard_map(
        body,
        mesh=mesh,
        in_specs=(spec,) * 5,
        out_specs=P(("layout", "tile", "chan"), None),
        check_vma=False,
    )
```

```python
import functools
import math

import jax
import jax.numpy as jnp
import numpy as np
from jax import lax
from jax.experimental import pallas as pl
from jax.experimental.pallas import tpu as pltpu
from jax.sharding import PartitionSpec as P

G = 4096
TILE = 64
CAP = 4
NT = 64
LANES = 128
QUARTERS = 4
ROWS = TILE // QUARTERS
BLOCKS = G // LANES
OUT_ROWS = 32
MESH = pl.DeviceIdType.MESH
VMEM_LIMIT = 16 * 2**20
F32 = jnp.float32
BF16 = jnp.bfloat16


def two_parts(table):
    table = np.asarray(table, np.float32)
    high = table.astype(BF16)
    low = (table - high.astype(np.float32)).astype(BF16)
    return np.concatenate([high, low], axis=0)


@functools.lru_cache
def tables(devices):
    spread = (np.arange(NT)[:, None] == np.arange(NT * CAP)[None, :] // CAP).astype(BF16)
    turn = 2.0 * np.pi * np.outer(np.arange(LANES), np.arange(LANES)) / LANES
    cos, sin = np.cos(turn), np.sin(turn)
    row_table = two_parts(np.block([[cos, -sin], [sin, cos]]))
    turn = 2.0 * np.pi * np.outer(np.arange(BLOCKS), np.arange(LANES)) / G
    row_twist = np.stack([np.cos(turn), np.sin(turn)]).astype(np.float32)
    wide = G // ROWS
    turn = 2.0 * np.pi * np.outer(np.arange(wide), np.arange(devices)) / wide
    cos, sin = np.cos(turn), np.sin(turn)
    col_table = two_parts(np.block([[cos, -sin], [sin, cos]]))
    turn = 2.0 * np.pi * np.outer(np.arange(wide), np.arange(LANES) % ROWS) / G
    col_twist = np.stack([np.cos(turn), np.sin(turn)]).astype(np.float32)
    group = LANES // ROWS
    out_index = np.arange(ROWS * group)
    lane = np.arange(LANES)
    same = (out_index[:, None] % group == lane[None, :] // ROWS) / math.sqrt(devices * NT * NT * CAP)
    turn = 2.0 * np.pi * np.outer(out_index // group, lane % ROWS) / ROWS
    last_table = two_parts(np.concatenate([same * np.cos(turn), -same * np.sin(turn)], axis=1))
    return spread, row_table, row_twist, col_table, col_twist, last_table


def split(value):
    high = value.astype(BF16)
    return high, (value - high.astype(F32)).astype(BF16)


def dot(left, right, right_dim):
    return lax.dot_general(left, right, (((1,), (right_dim,)), ((), ())), preferred_element_type=F32)


def table_dot(table, value, right_dim):
    high, low = split(value)
    half = table.shape[0] // 2
    both = dot(table[...], high, right_dim)
    return both[:half] + both[half:] + dot(table[:half], low, right_dim)


def times(value, real, imag):
    v_re, v_im = value
    if abs(imag) < 1e-12:
        if abs(real - 1.0) < 1e-12:
            return value
        return v_re * real, None if v_im is None else v_im * real
    if v_im is None:
        return (None if abs(real) < 1e-12 else v_re * real), v_re * imag
    if abs(real) < 1e-12:
        return -v_im * imag, v_re * imag
    return v_re * real - v_im * imag, v_re * imag + v_im * real


def plus(a, b, sign):
    if b is None:
        return a
    if a is None:
        return b if sign > 0 else -b
    return a + b if sign > 0 else a - b


def real_transform(values):
    count = len(values)
    if count == 1:
        return [(values[0], None)]
    if count == 2:
        return [(values[0] + values[1], None), (values[0] - values[1], None)]
    even, odd = real_transform(values[0::2]), real_transform(values[1::2])
    out = [None] * (count // 2 + 1)
    for k in range(count // 4 + 1):
        turn = 2.0 * math.pi * k / count
        turned = times(odd[k], math.cos(turn), math.sin(turn))
        out[k] = (plus(even[k][0], turned[0], 1), plus(even[k][1], turned[1], 1))
        far_im = plus(even[k][1], turned[1], -1)
        out[count // 2 - k] = (plus(even[k][0], turned[0], -1), None if far_im is None else -far_im)
    return out


def far_chips_first(side):
    half = side // 2
    ties = [step for j in range(side) for step in ([(half, j), (j, half)] if j != half else [(half, half)])]
    quarter = [(a, b) for a in range(half - 1, 0, -1) for b in range(half - 1, -1, -1)]
    quarter.sort(key=lambda step: -sum(step))
    turned = [step for a, b in quarter for step in ((a, b), (-b, a), (-a, -b), (b, -a))]
    return [(dx % side, dy % side) for dx, dy in ties + turned]


def kernel(tiles, chans, *refs):
    operands, columns, refs = refs[:8], refs[8], refs[9:]
    weight, frac_u, frac_v, code, fill, spread, row_table, row_twist = refs[:8]
    sample, packed, middle, landed, sorted_, slab, rows, high, low, spectrum = refs[8:18]
    load, send_1, recv_1, send_2, recv_2, send_x, recv_x, send_b, recv_b = refs[18:]
    side = math.isqrt(tiles)
    count = tiles * chans
    layout, tile, chan = lax.axis_index("layout"), lax.axis_index("tile"), lax.axis_index("chan")
    x, y = lax.div(tile, side), lax.rem(tile, side)
    along, across = jnp.where(chan == 0, x, y), jnp.where(chan == 0, y, x)
    me = tile * chans + chan
    mine = lax.rem(me, QUARTERS)
    far_first = sorted(range(side), key=lambda d: -min(d, side - d))

    def ahead(value, step):
        if step == 0:
            return value
        value = value + step
        return jnp.where(value >= side, value - side, value)

    def place(to_x, to_y, to_chan):
        return (layout, to_x * side + to_y, to_chan)

    def turned_place(to_along, to_across, to_chan):
        return place(
            jnp.where(chan == 0, to_along, to_across), jnp.where(chan == 0, to_across, to_along), to_chan
        )

    def send(src, dst, send_sem, recv_sem, device):
        pltpu.make_async_remote_copy(
            src_ref=src,
            dst_ref=dst,
            send_sem=send_sem,
            recv_sem=recv_sem,
            device_id=device,
            device_id_type=MESH,
        ).start()

    def await_bytes(ref, sem):
        pltpu.make_async_copy(ref, ref, sem).wait()

    loads = [
        pltpu.make_async_copy(src, dst, load.at[k])
        for k, (src, dst) in enumerate(zip(operands, refs[:8], strict=True))
    ]
    for k in (4, 5, 0, 3, 1, 2, 6, 7):
        loads[k].start()

    steps = [d for d in far_first if d != 0]
    barrier = pltpu.get_barrier_semaphore()
    senders = [turned_place(ahead(along, d), across, e) for d in steps for e in range(chans)]
    senders += [turned_place(along, ahead(across, d), chan) for d in steps]
    senders += [place(x, y, 1 - chan)]
    for device in senders:
        pl.semaphore_signal(barrier, inc=1, device_id=device, device_id_type=MESH)

    for k in range(6):
        loads[k].wait()

    fill_wide = dot(fill[0].astype(F32).astype(BF16), spread[...], 0)
    slot = lax.broadcasted_iota(jnp.int32, (NT, NT * CAP), 1) % CAP
    sample[0] = jnp.where(slot.astype(F32) < fill_wide, weight[0], 0.0)
    far = lax.broadcasted_iota(jnp.int32, (NT, NT * CAP), 0) >= NT // 2
    for part, position in (
        (1, (code[0] >> 6).astype(F32) + frac_u[0]),
        (2, (code[0] & (TILE - 1)).astype(F32) + frac_v[0]),
    ):
        sample[part] = jnp.where(far, TILE - position, position) * 0.25

    lower = lax.broadcasted_iota(jnp.int32, (1, LANES), 1) < LANES // 2

    @pl.loop(0, side)
    def _(to_x):
        for near_y in range(side // 2):
            p = to_x * (side // 2) + near_y
            for part in range(3):
                near = sample[part, pl.ds(p, 1), :]
                away = sample[part, pl.ds(NT - 1 - p, 1), :]
                for q in range(QUARTERS):
                    a = near[:, (q // 2) * LANES : (q // 2 + 1) * LANES]
                    b = away[:, (1 - q // 2) * LANES : (2 - q // 2) * LANES]
                    if q % 2 == 0:
                        row = jnp.where(lower, a, b)
                    else:
                        row = pltpu.roll(jnp.where(lower, b, a), LANES // 2, 1)
                    to_y, to_chan = 2 * near_y + q // 2, q % 2
                    where = to_x * side + to_y if to_chan == 0 else tiles + to_y * side + to_x
                    packed[where, pl.ds(part, 1), :] = row

    pl.semaphore_wait(barrier, len(senders))

    def strand(start):
        return packed.at[pl.ds(start * side, side)]

    for d in steps:
        to_x, to_y = ahead(x, d), ahead(y, d)
        send(strand(to_x), middle.at[:, x * chans + chan], send_1, recv_1, place(to_x, y, 0))
        send(strand(side + to_y), middle.at[:, y * chans + chan], send_1, recv_1, place(x, to_y, 1))
    send(
        strand(jnp.where(chan == 0, side + y, x)),
        middle.at[:, across * chans + chan],
        send_1,
        recv_1,
        place(x, y, 1 - chan),
    )
    middle[:, along * chans + chan] = packed[pl.ds((chan * side + along) * side, side)]
    await_bytes(packed.at[pl.ds(0, (2 * side - 1) * side)], recv_1)
    for d in steps:
        to = ahead(across, d)
        send(middle.at[to], landed.at[across], send_2, recv_2, turned_place(along, to, chan))
    landed[across] = middle[across]
    await_bytes(landed.at[pl.ds(0, side - 1)], recv_2)

    for part in range(3):
        sorted_[part] = landed[:, :, part, :].reshape(count, LANES).T

    cell = lax.broadcasted_iota(jnp.int32, (TILE, count), 0).astype(F32) * 0.25

    def taper(row, where):
        scaled = cell - row[where]
        inner = jnp.maximum(1.0 - scaled * scaled, 0.0)
        return inner * inner

    def one_tile(k):
        total = jnp.zeros((2 * TILE, 2 * TILE), F32)
        starts = [CAP * k, NT * CAP // 2 - CAP - CAP * k]
        for start in starts:
            for pair in range(CAP // 2):
                lefts, rights = [], []
                for slot in range(2):
                    where = pl.ds(start + 2 * pair + slot, 1)
                    u_high, u_low = split(taper(sorted_.at[1], where) * sorted_[0, where])
                    v_high, v_low = split(taper(sorted_.at[2], where))
                    lefts.append(jnp.concatenate([u_high, u_low], axis=0))
                    rights.append(jnp.concatenate([v_high, v_low], axis=0))
                total += dot(jnp.concatenate(lefts, axis=1), jnp.concatenate(rights, axis=1), 1)
        return total[:TILE] + total[TILE:]

    upper_half = lax.broadcasted_iota(jnp.int32, (TILE, LANES), 1) >= TILE
    strip = BLOCKS // QUARTERS
    others = []
    for hop in range(1, QUARTERS):
        other = lax.rem(mine + hop, QUARTERS)
        index = me - mine + other
        others.append((other, (layout, lax.div(index, chans), lax.rem(index, chans))))

    def row_range(index):
        return pl.ds(pl.multiple_of(index * ROWS, ROWS), ROWS)

    for pair in range(strip):
        first, second = one_tile(2 * pair), one_tile(2 * pair + 1)
        first = first + pltpu.roll(first, TILE, 1)
        second = second + pltpu.roll(second, TILE, 1)
        slab[pair] = jnp.where(upper_half, second, first)
        for other, device in others:
            send(slab.at[pair, row_range(other), :], rows.at[mine * strip + pair], send_x, recv_x, device)

    rows[pl.ds(mine * strip, strip)] = slab[:, row_range(mine), :]
    for k in (6, 7):
        loads[k].wait()
    await_bytes(rows.at[pl.ds(0, BLOCKS - strip)], recv_x)

    waves = real_transform([rows[t] for t in range(BLOCKS)])
    for k in range(BLOCKS):
        re, im = waves[min(k, BLOCKS - k)]
        c, s = row_twist[0, k : k + 1, :], row_twist[1, k : k + 1, :]
        if im is None:
            turned = (re * c, re * s)
        elif k <= BLOCKS // 2:
            turned = (re * c - im * s, re * s + im * c)
        else:
            turned = (re * c + im * s, re * s - im * c)
        for part in range(2):
            upper, rest = split(turned[part])
            high[ROWS * k : ROWS * (k + 1), LANES * part : LANES * (part + 1)] = upper
            low[ROWS * k : ROWS * (k + 1), LANES * part : LANES * (part + 1)] = rest
    groups = BLOCKS * ROWS // LANES
    for lane in range(0, groups, 2):
        where = slice(LANES * lane, LANES * (lane + 2))
        both = dot(row_table[...], high[where], 1)
        half = 2 * LANES
        both = both[:half] + both[half:] + dot(row_table[:half], low[where], 1)
        for part in range(2):
            for extra in range(2):
                spectrum[pl.ds(part * groups + lane + extra, count, stride=2 * groups), :] = both[
                    part * LANES : (part + 1) * LANES, extra * LANES : (extra + 1) * LANES
                ]

    each = 2 * groups

    def block(ref, index):
        return ref.at[pl.ds(pl.multiple_of(index * each, each), each), :]

    def send_column(to_x, to_y, same_chip=False):
        for e in range(1 if same_chip else 0, chans):
            to_chan = chan if e == 0 else 1 - chan
            to = (to_x * side + to_y) * chans + to_chan
            send(block(spectrum, to), block(columns, me), send_b, recv_b, place(to_x, to_y, to_chan))

    for dx, dy in far_chips_first(side):
        send_column(ahead(x, dx), ahead(y, dy))
    send_column(x, y, same_chip=True)

    own = pltpu.make_async_copy(block(spectrum, me), block(columns, me), load.at[0])
    own.start()
    own.wait()
    await_bytes(columns.at[pl.ds(0, (count - 1) * each), :], recv_b)
    await_bytes(packed.at[pl.ds(0, (2 * side - 1) * side)], send_1)
    await_bytes(landed.at[pl.ds(0, side - 1)], send_2)
    await_bytes(rows.at[pl.ds(0, BLOCKS - strip)], send_x)
    await_bytes(columns.at[pl.ds(0, (count - 1) * each), :], send_b)


def column_kernel(columns, col_table, col_twist, last_table, out, image, sem):
    count = col_table.shape[1] // 2
    each = columns.shape[0] // count
    groups, wide, tall = each // 2, G // ROWS, LANES // ROWS
    stores = []
    for pair in range(0, groups, 2):
        parts = [
            [columns[pl.ds(part * groups + pair + extra, count, stride=each), :] for part in range(2)]
            for extra in range(2)
        ]
        stacked = jnp.concatenate([jnp.concatenate(part, axis=0) for part in parts], axis=1)
        first = table_dot(col_table, stacked, 0)
        c, s = col_twist[0], col_twist[1]
        for extra in range(2):
            lane = pair + extra
            re = first[:wide, extra * LANES : (extra + 1) * LANES]
            im = first[wide:, extra * LANES : (extra + 1) * LANES]
            turned = jnp.concatenate([re * c - im * s, re * s + im * c], axis=1)
            last = table_dot(last_table, turned, 1)
            for l2 in range(ROWS):
                image[tall * lane : tall * (lane + 1), wide * l2 : wide * (l2 + 1)] = last[tall * l2 : tall * (l2 + 1)]
            here = pl.ds(tall * lane, tall)
            stores.append(pltpu.make_async_copy(image.at[here, :], out.at[here, :], sem.at[lane]))
            stores[-1].start()
    for store in stores:
        store.wait()


def body(*inputs):
    tiles, chans = lax.axis_size("tile"), lax.axis_size("chan")
    count, side = tiles * chans, math.isqrt(tiles)
    constants = [jnp.asarray(table) for table in tables(count)]
    operands = [pltpu.with_memory_space_constraint(v, pltpu.HBM) for v in [*inputs, *constants[:3]]]
    columns = pl.pallas_call(
        functools.partial(kernel, tiles, chans),
        out_shape=jax.ShapeDtypeStruct((count * 8, LANES), F32),
        in_specs=[pl.BlockSpec(memory_space=pltpu.HBM)] * len(operands),
        out_specs=pl.BlockSpec(memory_space=pl.ANY),
        scratch_shapes=[pltpu.VMEM(operand.shape, operand.dtype) for operand in operands]
        + [
            pltpu.VMEM((3, NT, NT * CAP), F32),
            pltpu.VMEM((count, 3, LANES), F32),
            pltpu.VMEM((side, side * chans, 3, LANES), F32),
            pltpu.VMEM((side, side * chans, 3, LANES), F32),
            pltpu.VMEM((3, LANES, count), F32),
            pltpu.VMEM((BLOCKS // QUARTERS, TILE, LANES), F32),
            pltpu.VMEM((BLOCKS, ROWS, LANES), F32),
            pltpu.VMEM((BLOCKS * ROWS, 2 * LANES), BF16),
            pltpu.VMEM((BLOCKS * ROWS, 2 * LANES), BF16),
            pltpu.VMEM((count * 8, LANES), F32),
            pltpu.SemaphoreType.DMA((len(operands),)),
        ]
        + [pltpu.SemaphoreType.DMA] * 8,
        compiler_params=pltpu.CompilerParams(
            collective_id=0, has_side_effects=True, vmem_limit_bytes=VMEM_LIMIT
        ),
    )(*operands)
    return pl.pallas_call(
        column_kernel,
        out_shape=jax.ShapeDtypeStruct((OUT_ROWS, G), F32),
        in_specs=[pl.BlockSpec(memory_space=pltpu.VMEM)] * 4,
        out_specs=pl.BlockSpec(memory_space=pl.ANY),
        scratch_shapes=[
            pltpu.VMEM((OUT_ROWS, G), F32),
            pltpu.SemaphoreType.DMA((BLOCKS * ROWS // LANES,)),
        ],
        compiler_params=pltpu.CompilerParams(vmem_limit_bytes=VMEM_LIMIT),
    )(columns, *constants[3:])


def solution(mesh):
    spec = P(("layout", "tile", "chan"), None, None)
    return jax.shard_map(
        body,
        mesh=mesh,
        in_specs=(spec,) * 5,
        out_specs=P(("layout", "tile", "chan"), None),
        check_vma=False,
    )
```

```python
import functools
import math

import jax
import jax.numpy as jnp
import numpy as np
from jax import lax
from jax.experimental import pallas as pl
from jax.experimental.pallas import tpu as pltpu
from jax.sharding import PartitionSpec as P

G = 4096
TILE = 64
CAP = 4
NT = 64
LANES = 128
QUARTERS = 4
ROWS = TILE // QUARTERS
BLOCKS = G // LANES
OUT_ROWS = 32
MESH = pl.DeviceIdType.MESH
VMEM_LIMIT = 16 * 2**20
F32 = jnp.float32
BF16 = jnp.bfloat16


def two_parts(table):
    table = np.asarray(table, np.float32)
    high = table.astype(BF16)
    low = (table - high.astype(np.float32)).astype(BF16)
    return np.concatenate([high, low], axis=0)


@functools.lru_cache
def tables(devices):
    spread = (np.arange(NT)[:, None] == np.arange(NT * CAP)[None, :] // CAP).astype(BF16)
    turn = 2.0 * np.pi * np.outer(np.arange(LANES), np.arange(LANES)) / LANES
    cos, sin = np.cos(turn), np.sin(turn)
    row_table = two_parts(np.block([[cos, -sin], [sin, cos]]))
    turn = 2.0 * np.pi * np.outer(np.arange(BLOCKS), np.arange(LANES)) / G
    row_twist = np.stack([np.cos(turn), np.sin(turn)]).astype(np.float32)
    wide = G // ROWS
    turn = 2.0 * np.pi * np.outer(np.arange(wide), np.arange(devices)) / wide
    cos, sin = np.cos(turn), np.sin(turn)
    col_table = two_parts(np.block([[cos, -sin], [sin, cos]]))
    turn = 2.0 * np.pi * np.outer(np.arange(wide), np.arange(LANES) % ROWS) / G
    col_twist = np.stack([np.cos(turn), np.sin(turn)]).astype(np.float32)
    group = LANES // ROWS
    out_index = np.arange(ROWS * group)
    lane = np.arange(LANES)
    same = (out_index[:, None] % group == lane[None, :] // ROWS) / math.sqrt(devices * NT * NT * CAP)
    turn = 2.0 * np.pi * np.outer(out_index // group, lane % ROWS) / ROWS
    last_table = two_parts(np.concatenate([same * np.cos(turn), -same * np.sin(turn)], axis=1))
    return spread, row_table, row_twist, col_table, col_twist, last_table


def split(value):
    high = value.astype(BF16)
    return high, (value - high.astype(F32)).astype(BF16)


def dot(left, right, right_dim):
    return lax.dot_general(left, right, (((1,), (right_dim,)), ((), ())), preferred_element_type=F32)


def table_dot(table, value, right_dim):
    high, low = split(value)
    half = table.shape[0] // 2
    both = dot(table[...], high, right_dim)
    return both[:half] + both[half:] + dot(table[:half], low, right_dim)


def times(value, real, imag):
    v_re, v_im = value
    if abs(imag) < 1e-12:
        if abs(real - 1.0) < 1e-12:
            return value
        return v_re * real, None if v_im is None else v_im * real
    if v_im is None:
        return (None if abs(real) < 1e-12 else v_re * real), v_re * imag
    if abs(real) < 1e-12:
        return -v_im * imag, v_re * imag
    return v_re * real - v_im * imag, v_re * imag + v_im * real


def plus(a, b, sign):
    if b is None:
        return a
    if a is None:
        return b if sign > 0 else -b
    return a + b if sign > 0 else a - b


def real_transform(values):
    count = len(values)
    if count == 1:
        return [(values[0], None)]
    if count == 2:
        return [(values[0] + values[1], None), (values[0] - values[1], None)]
    even, odd = real_transform(values[0::2]), real_transform(values[1::2])
    out = [None] * (count // 2 + 1)
    for k in range(count // 4 + 1):
        turn = 2.0 * math.pi * k / count
        turned = times(odd[k], math.cos(turn), math.sin(turn))
        out[k] = (plus(even[k][0], turned[0], 1), plus(even[k][1], turned[1], 1))
        far_im = plus(even[k][1], turned[1], -1)
        out[count // 2 - k] = (plus(even[k][0], turned[0], -1), None if far_im is None else -far_im)
    return out


def far_chips_first(side):
    half = side // 2
    ties = [step for j in range(side) for step in ([(half, j), (j, half)] if j != half else [(half, half)])]
    quarter = [(a, b) for a in range(half - 1, 0, -1) for b in range(half - 1, -1, -1)]
    quarter.sort(key=lambda step: -sum(step))
    turned = [step for a, b in quarter for step in ((a, b), (-b, a), (-a, -b), (b, -a))]
    return [(dx % side, dy % side) for dx, dy in ties + turned]


def kernel(tiles, chans, *refs):
    operands, columns, refs = refs[:8], refs[8], refs[9:]
    weight, frac_u, frac_v, code, fill, spread, row_table, row_twist = refs[:8]
    sample, packed, middle, landed, sorted_, slab, rows, high, low, spectrum = refs[8:18]
    load, send_1, recv_1, send_2, recv_2, send_x, recv_x, send_b, recv_b = refs[18:]
    side = math.isqrt(tiles)
    count = tiles * chans
    layout, tile, chan = lax.axis_index("layout"), lax.axis_index("tile"), lax.axis_index("chan")
    x, y = lax.div(tile, side), lax.rem(tile, side)
    along, across = jnp.where(chan == 0, x, y), jnp.where(chan == 0, y, x)
    me = tile * chans + chan
    mine = lax.rem(me, QUARTERS)
    far_first = sorted(range(side), key=lambda d: -min(d, side - d))

    def ahead(value, step):
        if step == 0:
            return value
        value = value + step
        return jnp.where(value >= side, value - side, value)

    def place(to_x, to_y, to_chan):
        return (layout, to_x * side + to_y, to_chan)

    def turned_place(to_along, to_across, to_chan):
        return place(
            jnp.where(chan == 0, to_along, to_across), jnp.where(chan == 0, to_across, to_along), to_chan
        )

    def send(src, dst, send_sem, recv_sem, device):
        pltpu.make_async_remote_copy(
            src_ref=src,
            dst_ref=dst,
            send_sem=send_sem,
            recv_sem=recv_sem,
            device_id=device,
            device_id_type=MESH,
        ).start()

    def await_bytes(ref, sem):
        pltpu.make_async_copy(ref, ref, sem).wait()

    loads = [
        pltpu.make_async_copy(src, dst, load.at[k])
        for k, (src, dst) in enumerate(zip(operands, refs[:8], strict=True))
    ]
    for k in (4, 5, 0, 3, 1, 2, 6, 7):
        loads[k].start()

    steps = [d for d in far_first if d != 0]
    barrier = pltpu.get_barrier_semaphore()
    senders = [turned_place(ahead(along, d), across, e) for d in steps for e in range(chans)]
    senders += [turned_place(along, ahead(across, d), chan) for d in steps]
    senders += [place(x, y, 1 - chan)]
    for device in senders:
        pl.semaphore_signal(barrier, inc=1, device_id=device, device_id_type=MESH)

    for k in range(6):
        loads[k].wait()

    fill_wide = dot(fill[0].astype(F32).astype(BF16), spread[...], 0)
    slot = lax.broadcasted_iota(jnp.int32, (NT, NT * CAP), 1) % CAP
    sample[0] = jnp.where(slot.astype(F32) < fill_wide, weight[0], 0.0)
    far = lax.broadcasted_iota(jnp.int32, (NT, NT * CAP), 0) >= NT // 2
    for part, position in (
        (1, (code[0] >> 6).astype(F32) + frac_u[0]),
        (2, (code[0] & (TILE - 1)).astype(F32) + frac_v[0]),
    ):
        sample[part] = jnp.where(far, TILE - position, position) * 0.25

    lower = lax.broadcasted_iota(jnp.int32, (1, LANES), 1) < LANES // 2

    @pl.loop(0, side)
    def _(to_x):
        for near_y in range(side // 2):
            p = to_x * (side // 2) + near_y
            for part in range(3):
                near = sample[part, pl.ds(p, 1), :]
                away = sample[part, pl.ds(NT - 1 - p, 1), :]
                for q in range(QUARTERS):
                    a = near[:, (q // 2) * LANES : (q // 2 + 1) * LANES]
                    b = away[:, (1 - q // 2) * LANES : (2 - q // 2) * LANES]
                    if q % 2 == 0:
                        row = jnp.where(lower, a, b)
                    else:
                        row = pltpu.roll(jnp.where(lower, b, a), LANES // 2, 1)
                    to_y, to_chan = 2 * near_y + q // 2, q % 2
                    where = to_x * side + to_y if to_chan == 0 else tiles + to_y * side + to_x
                    packed[where, pl.ds(part, 1), :] = row

    pl.semaphore_wait(barrier, len(senders))

    def strand(start):
        return packed.at[pl.ds(start * side, side)]

    for d in steps:
        to_x, to_y = ahead(x, d), ahead(y, d)
        send(strand(to_x), middle.at[:, x * chans + chan], send_1, recv_1, place(to_x, y, 0))
        send(strand(side + to_y), middle.at[:, y * chans + chan], send_1, recv_1, place(x, to_y, 1))
    send(
        strand(jnp.where(chan == 0, side + y, x)),
        middle.at[:, across * chans + chan],
        send_1,
        recv_1,
        place(x, y, 1 - chan),
    )
    middle[:, along * chans + chan] = packed[pl.ds((chan * side + along) * side, side)]
    await_bytes(packed.at[pl.ds(0, (2 * side - 1) * side)], recv_1)
    for d in steps:
        to = ahead(across, d)
        send(middle.at[to], landed.at[across], send_2, recv_2, turned_place(along, to, chan))
    landed[across] = middle[across]
    await_bytes(landed.at[pl.ds(0, side - 1)], recv_2)

    for part in range(3):
        sorted_[part] = landed[:, :, part, :].reshape(count, LANES).T

    cell = lax.broadcasted_iota(jnp.int32, (TILE, count), 0).astype(F32) * 0.25

    def taper(row, where):
        scaled = cell - row[where]
        inner = jnp.maximum(1.0 - scaled * scaled, 0.0)
        return inner * inner

    def one_tile(k):
        total = jnp.zeros((2 * TILE, 2 * TILE), F32)
        starts = [CAP * k, NT * CAP // 2 - CAP - CAP * k]
        for start in starts:
            for pair in range(CAP // 2):
                lefts, rights = [], []
                for slot in range(2):
                    where = pl.ds(start + 2 * pair + slot, 1)
                    u_high, u_low = split(taper(sorted_.at[1], where) * sorted_[0, where])
                    v_high, v_low = split(taper(sorted_.at[2], where))
                    lefts.append(jnp.concatenate([u_high, u_low], axis=0))
                    rights.append(jnp.concatenate([v_high, v_low], axis=0))
                total += dot(jnp.concatenate(lefts, axis=1), jnp.concatenate(rights, axis=1), 1)
        return total[:TILE] + total[TILE:]

    upper_half = lax.broadcasted_iota(jnp.int32, (TILE, LANES), 1) >= TILE
    strip = BLOCKS // QUARTERS
    others = []
    for hop in range(1, QUARTERS):
        other = lax.rem(mine + hop, QUARTERS)
        index = me - mine + other
        others.append((other, (layout, lax.div(index, chans), lax.rem(index, chans))))

    def row_range(index):
        return pl.ds(pl.multiple_of(index * ROWS, ROWS), ROWS)

    cuts = (3 * strip // 4, strip)
    for pair in range(strip):
        first, second = one_tile(2 * pair), one_tile(2 * pair + 1)
        first = first + pltpu.roll(first, TILE, 1)
        second = second + pltpu.roll(second, TILE, 1)
        slab[pair] = jnp.where(upper_half, second, first)
        if pair + 1 in cuts:
            first = max([0] + [cut for cut in cuts if cut <= pair])
            some = pair + 1 - first
            for other, device in others:
                send(
                    slab.at[pl.ds(first, some), row_range(other), :],
                    rows.at[pl.ds(mine * strip + first, some)],
                    send_x,
                    recv_x,
                    device,
                )

    rows[pl.ds(mine * strip, strip)] = slab[:, row_range(mine), :]
    for k in (6, 7):
        loads[k].wait()
    await_bytes(rows.at[pl.ds(0, BLOCKS - strip)], recv_x)

    waves = real_transform([rows[t] for t in range(BLOCKS)])
    for k in range(BLOCKS):
        re, im = waves[min(k, BLOCKS - k)]
        c, s = row_twist[0, k : k + 1, :], row_twist[1, k : k + 1, :]
        if im is None:
            turned = (re * c, re * s)
        elif k <= BLOCKS // 2:
            turned = (re * c - im * s, re * s + im * c)
        else:
            turned = (re * c + im * s, re * s - im * c)
        for part in range(2):
            upper, rest = split(turned[part])
            high[ROWS * k : ROWS * (k + 1), LANES * part : LANES * (part + 1)] = upper
            low[ROWS * k : ROWS * (k + 1), LANES * part : LANES * (part + 1)] = rest
    groups = BLOCKS * ROWS // LANES
    for lane in range(0, groups, 2):
        where = slice(LANES * lane, LANES * (lane + 2))
        both = dot(row_table[...], high[where], 1)
        half = 2 * LANES
        both = both[:half] + both[half:] + dot(row_table[:half], low[where], 1)
        for part in range(2):
            for extra in range(2):
                spectrum[pl.ds(part * groups + lane + extra, count, stride=2 * groups), :] = both[
                    part * LANES : (part + 1) * LANES, extra * LANES : (extra + 1) * LANES
                ]

    each = 2 * groups

    def block(ref, index):
        return ref.at[pl.ds(pl.multiple_of(index * each, each), each), :]

    def send_column(to_x, to_y, same_chip=False):
        for e in range(1 if same_chip else 0, chans):
            to_chan = chan if e == 0 else 1 - chan
            to = (to_x * side + to_y) * chans + to_chan
            send(block(spectrum, to), block(columns, me), send_b, recv_b, place(to_x, to_y, to_chan))

    for dx, dy in far_chips_first(side):
        send_column(ahead(x, dx), ahead(y, dy))
    send_column(x, y, same_chip=True)

    own = pltpu.make_async_copy(block(spectrum, me), block(columns, me), load.at[0])
    own.start()
    own.wait()
    await_bytes(columns.at[pl.ds(0, (count - 1) * each), :], recv_b)
    await_bytes(packed.at[pl.ds(0, (2 * side - 1) * side)], send_1)
    await_bytes(landed.at[pl.ds(0, side - 1)], send_2)
    await_bytes(rows.at[pl.ds(0, BLOCKS - strip)], send_x)
    await_bytes(columns.at[pl.ds(0, (count - 1) * each), :], send_b)


def column_kernel(columns, col_table, col_twist, last_table, out, image, sem):
    count = col_table.shape[1] // 2
    each = columns.shape[0] // count
    groups, wide, tall = each // 2, G // ROWS, LANES // ROWS
    stores = []
    for pair in range(0, groups, 2):
        parts = [
            [columns[pl.ds(part * groups + pair + extra, count, stride=each), :] for part in range(2)]
            for extra in range(2)
        ]
        stacked = jnp.concatenate([jnp.concatenate(part, axis=0) for part in parts], axis=1)
        first = table_dot(col_table, stacked, 0)
        c, s = col_twist[0], col_twist[1]
        for extra in range(2):
            lane = pair + extra
            re = first[:wide, extra * LANES : (extra + 1) * LANES]
            im = first[wide:, extra * LANES : (extra + 1) * LANES]
            turned = jnp.concatenate([re * c - im * s, re * s + im * c], axis=1)
            last = table_dot(last_table, turned, 1)
            for l2 in range(ROWS):
                image[tall * lane : tall * (lane + 1), wide * l2 : wide * (l2 + 1)] = last[tall * l2 : tall * (l2 + 1)]
            here = pl.ds(tall * lane, tall)
            stores.append(pltpu.make_async_copy(image.at[here, :], out.at[here, :], sem.at[lane]))
            stores[-1].start()
    for store in stores:
        store.wait()


def body(*inputs):
    tiles, chans = lax.axis_size("tile"), lax.axis_size("chan")
    count, side = tiles * chans, math.isqrt(tiles)
    constants = [jnp.asarray(table) for table in tables(count)]
    operands = [pltpu.with_memory_space_constraint(v, pltpu.HBM) for v in [*inputs, *constants[:3]]]
    columns = pl.pallas_call(
        functools.partial(kernel, tiles, chans),
        out_shape=jax.ShapeDtypeStruct((count * 8, LANES), F32),
        in_specs=[pl.BlockSpec(memory_space=pltpu.HBM)] * len(operands),
        out_specs=pl.BlockSpec(memory_space=pl.ANY),
        scratch_shapes=[pltpu.VMEM(operand.shape, operand.dtype) for operand in operands]
        + [
            pltpu.VMEM((3, NT, NT * CAP), F32),
            pltpu.VMEM((count, 3, LANES), F32),
            pltpu.VMEM((side, side * chans, 3, LANES), F32),
            pltpu.VMEM((side, side * chans, 3, LANES), F32),
            pltpu.VMEM((3, LANES, count), F32),
            pltpu.VMEM((BLOCKS // QUARTERS, TILE, LANES), F32),
            pltpu.VMEM((BLOCKS, ROWS, LANES), F32),
            pltpu.VMEM((BLOCKS * ROWS, 2 * LANES), BF16),
            pltpu.VMEM((BLOCKS * ROWS, 2 * LANES), BF16),
            pltpu.VMEM((count * 8, LANES), F32),
            pltpu.SemaphoreType.DMA((len(operands),)),
        ]
        + [pltpu.SemaphoreType.DMA] * 8,
        compiler_params=pltpu.CompilerParams(
            collective_id=0, has_side_effects=True, vmem_limit_bytes=VMEM_LIMIT
        ),
    )(*operands)
    return pl.pallas_call(
        column_kernel,
        out_shape=jax.ShapeDtypeStruct((OUT_ROWS, G), F32),
        in_specs=[pl.BlockSpec(memory_space=pltpu.VMEM)] * 4,
        out_specs=pl.BlockSpec(memory_space=pl.ANY),
        scratch_shapes=[
            pltpu.VMEM((OUT_ROWS, G), F32),
            pltpu.SemaphoreType.DMA((BLOCKS * ROWS // LANES,)),
        ],
        compiler_params=pltpu.CompilerParams(vmem_limit_bytes=VMEM_LIMIT),
    )(columns, *constants[3:])


def solution(mesh):
    spec = P(("layout", "tile", "chan"), None, None)
    return jax.shard_map(
        body,
        mesh=mesh,
        in_specs=(spec,) * 5,
        out_specs=P(("layout", "tile", "chan"), None),
        check_vma=False,
    )
```

```python
import functools
import math

import jax
import jax.numpy as jnp
import numpy as np
from jax import lax
from jax.experimental import pallas as pl
from jax.experimental.pallas import tpu as pltpu
from jax.sharding import PartitionSpec as P

G = 4096
TILE = 64
CAP = 4
NT = 64
LANES = 128
QUARTERS = 4
ROWS = TILE // QUARTERS
BLOCKS = G // LANES
OUT_ROWS = 32
MESH = pl.DeviceIdType.MESH
VMEM_LIMIT = 16 * 2**20
F32 = jnp.float32
BF16 = jnp.bfloat16


def two_parts(table):
    table = np.asarray(table, np.float32)
    high = table.astype(BF16)
    low = (table - high.astype(np.float32)).astype(BF16)
    return np.concatenate([high, low], axis=0)


@functools.lru_cache
def tables(devices):
    spread = (np.arange(NT)[:, None] == np.arange(NT * CAP)[None, :] // CAP).astype(BF16)
    turn = 2.0 * np.pi * np.outer(np.arange(LANES), np.arange(LANES)) / LANES
    cos, sin = np.cos(turn), np.sin(turn)
    row_table = two_parts(np.block([[cos, -sin], [sin, cos]]))
    turn = 2.0 * np.pi * np.outer(np.arange(BLOCKS), np.arange(LANES)) / G
    row_twist = np.stack([np.cos(turn), np.sin(turn)]).astype(np.float32)
    wide = G // ROWS
    turn = 2.0 * np.pi * np.outer(np.arange(wide), np.arange(devices)) / wide
    cos, sin = np.cos(turn), np.sin(turn)
    col_table = two_parts(np.block([[cos, -sin], [sin, cos]]))
    turn = 2.0 * np.pi * np.outer(np.arange(wide), np.arange(LANES) % ROWS) / G
    col_twist = np.stack([np.cos(turn), np.sin(turn)]).astype(np.float32)
    group = LANES // ROWS
    out_index = np.arange(ROWS * group)
    lane = np.arange(LANES)
    same = (out_index[:, None] % group == lane[None, :] // ROWS) / math.sqrt(devices * NT * NT * CAP)
    turn = 2.0 * np.pi * np.outer(out_index // group, lane % ROWS) / ROWS
    last_table = two_parts(np.concatenate([same * np.cos(turn), -same * np.sin(turn)], axis=1))
    return spread, row_table, row_twist, col_table, col_twist, last_table


def split(value):
    high = value.astype(BF16)
    return high, (value - high.astype(F32)).astype(BF16)


def dot(left, right, right_dim):
    return lax.dot_general(left, right, (((1,), (right_dim,)), ((), ())), preferred_element_type=F32)


def table_dot(table, high, low, right_dim):
    half = table.shape[0] // 2
    return dot(table[:half], high, right_dim) + dot(table[half:], high, right_dim) + dot(table[:half], low, right_dim)


def times(value, real, imag):
    v_re, v_im = value
    if abs(imag) < 1e-12:
        if abs(real - 1.0) < 1e-12:
            return value
        return v_re * real, None if v_im is None else v_im * real
    if v_im is None:
        return (None if abs(real) < 1e-12 else v_re * real), v_re * imag
    if abs(real) < 1e-12:
        return -v_im * imag, v_re * imag
    return v_re * real - v_im * imag, v_re * imag + v_im * real


def plus(a, b, sign):
    if b is None:
        return a
    if a is None:
        return b if sign > 0 else -b
    return a + b if sign > 0 else a - b


def real_transform(values):
    count = len(values)
    if count == 1:
        return [(values[0], None)]
    if count == 2:
        return [(values[0] + values[1], None), (values[0] - values[1], None)]
    even, odd = real_transform(values[0::2]), real_transform(values[1::2])
    out = [None] * (count // 2 + 1)
    for k in range(count // 4 + 1):
        turn = 2.0 * math.pi * k / count
        turned = times(odd[k], math.cos(turn), math.sin(turn))
        out[k] = (plus(even[k][0], turned[0], 1), plus(even[k][1], turned[1], 1))
        far_im = plus(even[k][1], turned[1], -1)
        out[count // 2 - k] = (plus(even[k][0], turned[0], -1), None if far_im is None else -far_im)
    return out


def far_chips_first(side):
    half = side // 2
    ties = [step for j in range(side) for step in ([(half, j), (j, half)] if j != half else [(half, half)])]
    quarter = [(a, b) for a in range(half - 1, 0, -1) for b in range(half - 1, -1, -1)]
    quarter.sort(key=lambda step: -sum(step))
    turned = [step for a, b in quarter for step in ((a, b), (-b, a), (-a, -b), (b, -a))]
    return [(dx % side, dy % side) for dx, dy in ties + turned]


def kernel(tiles, chans, *refs):
    operands, columns, refs = refs[:8], refs[8], refs[9:]
    weight, frac_u, frac_v, code, fill, spread, row_table, row_twist = refs[:8]
    sample, packed, middle, landed, sorted_, slab, rows, high, low, spectrum = refs[8:18]
    load, send_1, recv_1, send_2, recv_2, send_x, recv_x, send_b, recv_b = refs[18:]
    side = math.isqrt(tiles)
    count = tiles * chans
    layout, tile, chan = lax.axis_index("layout"), lax.axis_index("tile"), lax.axis_index("chan")
    x, y = lax.div(tile, side), lax.rem(tile, side)
    along, across = jnp.where(chan == 0, x, y), jnp.where(chan == 0, y, x)
    me = tile * chans + chan
    mine = lax.rem(me, QUARTERS)
    far_first = sorted(range(side), key=lambda d: -min(d, side - d))

    def ahead(value, step):
        if step == 0:
            return value
        value = value + step
        return jnp.where(value >= side, value - side, value)

    def place(to_x, to_y, to_chan):
        return (layout, to_x * side + to_y, to_chan)

    def turned_place(to_along, to_across, to_chan):
        return place(
            jnp.where(chan == 0, to_along, to_across), jnp.where(chan == 0, to_across, to_along), to_chan
        )

    def send(src, dst, send_sem, recv_sem, device):
        pltpu.make_async_remote_copy(
            src_ref=src,
            dst_ref=dst,
            send_sem=send_sem,
            recv_sem=recv_sem,
            device_id=device,
            device_id_type=MESH,
        ).start()

    def await_bytes(ref, sem):
        pltpu.make_async_copy(ref, ref, sem).wait()

    loads = [
        pltpu.make_async_copy(src, dst, load.at[k])
        for k, (src, dst) in enumerate(zip(operands, refs[:8], strict=True))
    ]
    for k in (4, 5, 0, 3, 1, 2, 6, 7):
        loads[k].start()

    steps = [d for d in far_first if d != 0]
    barrier = pltpu.get_barrier_semaphore()
    senders = [turned_place(ahead(along, d), across, e) for d in steps for e in range(chans)]
    senders += [turned_place(along, ahead(across, d), chan) for d in steps]
    senders += [place(x, y, 1 - chan)]
    for device in senders:
        pl.semaphore_signal(barrier, inc=1, device_id=device, device_id_type=MESH)

    for k in range(6):
        loads[k].wait()

    fill_wide = dot(fill[0].astype(F32).astype(BF16), spread[...], 0)
    slot = lax.broadcasted_iota(jnp.int32, (NT, NT * CAP), 1) % CAP
    sample[0] = jnp.where(slot.astype(F32) < fill_wide, weight[0], 0.0)
    far = lax.broadcasted_iota(jnp.int32, (NT, NT * CAP), 0) >= NT // 2
    for part, position in (
        (1, (code[0] >> 6).astype(F32) + frac_u[0]),
        (2, (code[0] & (TILE - 1)).astype(F32) + frac_v[0]),
    ):
        sample[part] = jnp.where(far, TILE - position, position) * 0.25

    lower = lax.broadcasted_iota(jnp.int32, (1, LANES), 1) < LANES // 2

    @pl.loop(0, side)
    def _(to_x):
        for near_y in range(side // 2):
            p = to_x * (side // 2) + near_y
            for part in range(3):
                near = sample[part, pl.ds(p, 1), :]
                away = sample[part, pl.ds(NT - 1 - p, 1), :]
                for q in range(QUARTERS):
                    a = near[:, (q // 2) * LANES : (q // 2 + 1) * LANES]
                    b = away[:, (1 - q // 2) * LANES : (2 - q // 2) * LANES]
                    if q % 2 == 0:
                        row = jnp.where(lower, a, b)
                    else:
                        row = pltpu.roll(jnp.where(lower, b, a), LANES // 2, 1)
                    to_y, to_chan = 2 * near_y + q // 2, q % 2
                    where = to_x * side + to_y if to_chan == 0 else tiles + to_y * side + to_x
                    packed[where, pl.ds(part, 1), :] = row

    pl.semaphore_wait(barrier, len(senders))

    def strand(start):
        return packed.at[pl.ds(start * side, side)]

    for d in steps:
        to_x, to_y = ahead(x, d), ahead(y, d)
        send(strand(to_x), middle.at[:, x * chans + chan], send_1, recv_1, place(to_x, y, 0))
        send(strand(side + to_y), middle.at[:, y * chans + chan], send_1, recv_1, place(x, to_y, 1))
    send(
        strand(jnp.where(chan == 0, side + y, x)),
        middle.at[:, across * chans + chan],
        send_1,
        recv_1,
        place(x, y, 1 - chan),
    )
    middle[:, along * chans + chan] = packed[pl.ds((chan * side + along) * side, side)]
    await_bytes(packed.at[pl.ds(0, (2 * side - 1) * side)], recv_1)
    for d in steps:
        to = ahead(across, d)
        send(middle.at[to], landed.at[across], send_2, recv_2, turned_place(along, to, chan))
    landed[across] = middle[across]
    await_bytes(landed.at[pl.ds(0, side - 1)], recv_2)

    for part in range(3):
        sorted_[part] = landed[:, :, part, :].reshape(count, LANES).T

    cell = lax.broadcasted_iota(jnp.int32, (TILE, count), 0).astype(F32) * 0.25

    def taper(row, where):
        scaled = cell - row[where]
        inner = jnp.maximum(1.0 - scaled * scaled, 0.0)
        return inner * inner

    def one_tile(k):
        total = jnp.zeros((2 * TILE, 2 * TILE), F32)
        starts = [CAP * k, NT * CAP // 2 - CAP - CAP * k]
        for start in starts:
            for pair in range(CAP // 2):
                lefts, rights = [], []
                for slot in range(2):
                    where = pl.ds(start + 2 * pair + slot, 1)
                    u_high, u_low = split(taper(sorted_.at[1], where) * sorted_[0, where])
                    v_high, v_low = split(taper(sorted_.at[2], where))
                    lefts.append(jnp.concatenate([u_high, u_low], axis=0))
                    rights.append(jnp.concatenate([v_high, v_low], axis=0))
                total += dot(jnp.concatenate(lefts, axis=1), jnp.concatenate(rights, axis=1), 1)
        return total[:TILE] + total[TILE:]

    upper_half = lax.broadcasted_iota(jnp.int32, (TILE, LANES), 1) >= TILE
    strip = BLOCKS // QUARTERS
    others = []
    for hop in (2, 3, 1):
        other = lax.rem(mine + hop, QUARTERS)
        index = me - mine + other
        others.append((other, (layout, lax.div(index, chans), lax.rem(index, chans))))

    def row_range(index):
        return pl.ds(pl.multiple_of(index * ROWS, ROWS), ROWS)

    cuts = (3 * strip // 4, strip)
    for pair in range(strip):
        first, second = one_tile(2 * pair), one_tile(2 * pair + 1)
        first = first + pltpu.roll(first, TILE, 1)
        second = second + pltpu.roll(second, TILE, 1)
        slab[pair] = jnp.where(upper_half, second, first)
        if pair + 1 in cuts:
            first = max([0] + [cut for cut in cuts if cut <= pair])
            some = pair + 1 - first
            for other, device in others:
                send(
                    slab.at[pl.ds(first, some), row_range(other), :],
                    rows.at[pl.ds(mine * strip + first, some)],
                    send_x,
                    recv_x,
                    device,
                )

    rows[pl.ds(mine * strip, strip)] = slab[:, row_range(mine), :]
    for k in (6, 7):
        loads[k].wait()
    await_bytes(rows.at[pl.ds(0, BLOCKS - strip)], recv_x)

    waves = real_transform([rows[t] for t in range(BLOCKS)])
    for k in range(BLOCKS):
        re, im = waves[min(k, BLOCKS - k)]
        c, s = row_twist[0, k : k + 1, :], row_twist[1, k : k + 1, :]
        if im is None:
            turned = (re * c, re * s)
        elif k <= BLOCKS // 2:
            turned = (re * c - im * s, re * s + im * c)
        else:
            turned = (re * c + im * s, re * s - im * c)
        for part in range(2):
            upper, rest = split(turned[part])
            high[ROWS * k : ROWS * (k + 1), LANES * part : LANES * (part + 1)] = upper
            low[ROWS * k : ROWS * (k + 1), LANES * part : LANES * (part + 1)] = rest
    groups = BLOCKS * ROWS // LANES
    for lane in range(0, groups, 2):
        where = slice(LANES * lane, LANES * (lane + 2))
        both = table_dot(row_table, high[where], low[where], 1)
        for part in range(2):
            for extra in range(2):
                spectrum[pl.ds(part * groups + lane + extra, count, stride=2 * groups), :] = both[
                    part * LANES : (part + 1) * LANES, extra * LANES : (extra + 1) * LANES
                ]

    each = 2 * groups

    def block(ref, index):
        return ref.at[pl.ds(pl.multiple_of(index * each, each), each), :]

    def send_column(to_x, to_y, same_chip=False):
        for e in range(1 if same_chip else 0, chans):
            to_chan = chan if e == 0 else 1 - chan
            to = (to_x * side + to_y) * chans + to_chan
            send(block(spectrum, to), block(columns, me), send_b, recv_b, place(to_x, to_y, to_chan))

    for dx, dy in far_chips_first(side):
        send_column(ahead(x, dx), ahead(y, dy))
    send_column(x, y, same_chip=True)

    own = pltpu.make_async_copy(block(spectrum, me), block(columns, me), load.at[0])
    own.start()
    own.wait()
    await_bytes(columns.at[pl.ds(0, (count - 1) * each), :], recv_b)
    await_bytes(packed.at[pl.ds(0, (2 * side - 1) * side)], send_1)
    await_bytes(landed.at[pl.ds(0, side - 1)], send_2)
    await_bytes(rows.at[pl.ds(0, BLOCKS - strip)], send_x)
    await_bytes(columns.at[pl.ds(0, (count - 1) * each), :], send_b)


def column_kernel(columns, col_table, col_twist, last_table, out, image, sem):
    count = col_table.shape[1] // 2
    each = columns.shape[0] // count
    groups, wide, tall = each // 2, G // ROWS, LANES // ROWS
    stores = []
    for pair in range(0, groups, 2):
        parts = [
            [columns[pl.ds(part * groups + pair + extra, count, stride=each), :] for part in range(2)]
            for extra in range(2)
        ]
        stacked = jnp.concatenate([jnp.concatenate(part, axis=0) for part in parts], axis=1)
        high, low = split(stacked)
        tops, ends = col_table[: 2 * wide], col_table[2 * wide :]
        real, imag = (
            table_dot(jnp.concatenate([tops[rows], ends[rows]], axis=0), high, low, 0)
            for rows in (slice(0, wide), slice(wide, 2 * wide))
        )
        c, s = col_twist[0], col_twist[1]
        for extra in range(2):
            lane = pair + extra
            re = real[:, extra * LANES : (extra + 1) * LANES]
            im = imag[:, extra * LANES : (extra + 1) * LANES]
            turned = jnp.concatenate([re * c - im * s, re * s + im * c], axis=1)
            high_turned, low_turned = split(turned)
            both = dot(last_table[...], high_turned, 1)
            half = last_table.shape[0] // 2
            last = both[:half] + both[half:] + dot(last_table[:half], low_turned, 1)
            for l2 in range(ROWS):
                image[tall * lane : tall * (lane + 1), wide * l2 : wide * (l2 + 1)] = last[tall * l2 : tall * (l2 + 1)]
            here = pl.ds(tall * lane, tall)
            stores.append(pltpu.make_async_copy(image.at[here, :], out.at[here, :], sem.at[lane]))
            stores[-1].start()
    for store in stores:
        store.wait()


def body(*inputs):
    tiles, chans = lax.axis_size("tile"), lax.axis_size("chan")
    count, side = tiles * chans, math.isqrt(tiles)
    constants = [jnp.asarray(table) for table in tables(count)]
    operands = [pltpu.with_memory_space_constraint(v, pltpu.HBM) for v in [*inputs, *constants[:3]]]
    columns = pl.pallas_call(
        functools.partial(kernel, tiles, chans),
        out_shape=jax.ShapeDtypeStruct((count * 8, LANES), F32),
        in_specs=[pl.BlockSpec(memory_space=pltpu.HBM)] * len(operands),
        out_specs=pl.BlockSpec(memory_space=pl.ANY),
        scratch_shapes=[pltpu.VMEM(operand.shape, operand.dtype) for operand in operands]
        + [
            pltpu.VMEM((3, NT, NT * CAP), F32),
            pltpu.VMEM((count, 3, LANES), F32),
            pltpu.VMEM((side, side * chans, 3, LANES), F32),
            pltpu.VMEM((side, side * chans, 3, LANES), F32),
            pltpu.VMEM((3, LANES, count), F32),
            pltpu.VMEM((BLOCKS // QUARTERS, TILE, LANES), F32),
            pltpu.VMEM((BLOCKS, ROWS, LANES), F32),
            pltpu.VMEM((BLOCKS * ROWS, 2 * LANES), BF16),
            pltpu.VMEM((BLOCKS * ROWS, 2 * LANES), BF16),
            pltpu.VMEM((count * 8, LANES), F32),
            pltpu.SemaphoreType.DMA((len(operands),)),
        ]
        + [pltpu.SemaphoreType.DMA] * 8,
        compiler_params=pltpu.CompilerParams(
            collective_id=0, has_side_effects=True, vmem_limit_bytes=VMEM_LIMIT
        ),
    )(*operands)
    return pl.pallas_call(
        column_kernel,
        out_shape=jax.ShapeDtypeStruct((OUT_ROWS, G), F32),
        in_specs=[pl.BlockSpec(memory_space=pltpu.VMEM)] * 4,
        out_specs=pl.BlockSpec(memory_space=pl.ANY),
        scratch_shapes=[
            pltpu.VMEM((OUT_ROWS, G), F32),
            pltpu.SemaphoreType.DMA((BLOCKS * ROWS // LANES,)),
        ],
        compiler_params=pltpu.CompilerParams(vmem_limit_bytes=VMEM_LIMIT),
    )(columns, *constants[3:])


def solution(mesh):
    spec = P(("layout", "tile", "chan"), None, None)
    return jax.shard_map(
        body,
        mesh=mesh,
        in_specs=(spec,) * 5,
        out_specs=P(("layout", "tile", "chan"), None),
        check_vma=False,
    )
```

```python
import functools
import math

import jax
import jax.numpy as jnp
import numpy as np
from jax import lax
from jax.experimental import pallas as pl
from jax.experimental.pallas import tpu as pltpu
from jax.sharding import PartitionSpec as P

G = 4096
TILE = 64
CAP = 4
NT = 64
LANES = 128
QUARTERS = 4
ROWS = TILE // QUARTERS
BLOCKS = G // LANES
OUT_ROWS = 32
MESH = pl.DeviceIdType.MESH
VMEM_LIMIT = 16 * 2**20
F32 = jnp.float32
BF16 = jnp.bfloat16


def two_parts(table):
    table = np.asarray(table, np.float32)
    high = table.astype(BF16)
    low = (table - high.astype(np.float32)).astype(BF16)
    return np.concatenate([high, low], axis=0)


@functools.lru_cache
def tables(devices):
    spread = (np.arange(NT)[:, None] == np.arange(NT * CAP)[None, :] // CAP).astype(BF16)
    turn = 2.0 * np.pi * np.outer(np.arange(LANES), np.arange(LANES)) / LANES
    cos, sin = np.cos(turn), np.sin(turn)
    row_table = two_parts(np.block([[cos, -sin], [sin, cos]]))
    turn = 2.0 * np.pi * np.outer(np.arange(BLOCKS), np.arange(LANES)) / G
    row_twist = np.stack([np.cos(turn), np.sin(turn)]).astype(np.float32)
    wide = G // ROWS
    turn = 2.0 * np.pi * np.outer(np.arange(wide), np.arange(devices)) / wide
    cos, sin = np.cos(turn), np.sin(turn)
    col_table = two_parts(np.block([[cos, -sin], [sin, cos]]))
    turn = 2.0 * np.pi * np.outer(np.arange(wide), np.arange(LANES) % ROWS) / G
    col_twist = np.stack([np.cos(turn), np.sin(turn)]).astype(np.float32)
    group = LANES // ROWS
    out_index = np.arange(ROWS * group)
    lane = np.arange(LANES)
    same = (out_index[:, None] % group == lane[None, :] // ROWS) / math.sqrt(devices * NT * NT * CAP)
    turn = 2.0 * np.pi * np.outer(out_index // group, lane % ROWS) / ROWS
    last_table = two_parts(np.concatenate([same * np.cos(turn), -same * np.sin(turn)], axis=1))
    return spread, row_table, row_twist, col_table, col_twist, last_table


def split(value):
    high = value.astype(BF16)
    return high, (value - high.astype(F32)).astype(BF16)


def dot(left, right, right_dim):
    return lax.dot_general(left, right, (((1,), (right_dim,)), ((), ())), preferred_element_type=F32)


def table_dot(table, high, low, right_dim):
    half = table.shape[0] // 2
    return dot(table[:half], high, right_dim) + dot(table[half:], high, right_dim) + dot(table[:half], low, right_dim)


def times(value, real, imag):
    v_re, v_im = value
    if abs(imag) < 1e-12:
        if abs(real - 1.0) < 1e-12:
            return value
        return v_re * real, None if v_im is None else v_im * real
    if v_im is None:
        return (None if abs(real) < 1e-12 else v_re * real), v_re * imag
    if abs(real) < 1e-12:
        return -v_im * imag, v_re * imag
    return v_re * real - v_im * imag, v_re * imag + v_im * real


def plus(a, b, sign):
    if b is None:
        return a
    if a is None:
        return b if sign > 0 else -b
    return a + b if sign > 0 else a - b


def real_transform(values):
    count = len(values)
    if count == 1:
        return [(values[0], None)]
    if count == 2:
        return [(values[0] + values[1], None), (values[0] - values[1], None)]
    even, odd = real_transform(values[0::2]), real_transform(values[1::2])
    out = [None] * (count // 2 + 1)
    for k in range(count // 4 + 1):
        turn = 2.0 * math.pi * k / count
        turned = times(odd[k], math.cos(turn), math.sin(turn))
        out[k] = (plus(even[k][0], turned[0], 1), plus(even[k][1], turned[1], 1))
        far_im = plus(even[k][1], turned[1], -1)
        out[count // 2 - k] = (plus(even[k][0], turned[0], -1), None if far_im is None else -far_im)
    return out


def far_chips_first(side):
    half = side // 2
    ties = [step for j in range(side) for step in ([(half, j), (j, half)] if j != half else [(half, half)])]
    quarter = [(a, b) for a in range(half - 1, 0, -1) for b in range(half - 1, -1, -1)]
    quarter.sort(key=lambda step: -sum(step))
    turned = [step for a, b in quarter for step in ((a, b), (-b, a), (-a, -b), (b, -a))]
    return [(dx % side, dy % side) for dx, dy in ties + turned]


def kernel(tiles, chans, *refs):
    operands, columns, refs = refs[:8], refs[8], refs[9:]
    weight, frac_u, frac_v, code, fill, spread, row_table, row_twist = refs[:8]
    sample, packed, middle, landed, sorted_, slab, rows, high, low, spectrum = refs[8:18]
    load, send_1, recv_1, send_2, recv_2, send_x, recv_x, send_b, recv_b = refs[18:]
    side = math.isqrt(tiles)
    count = tiles * chans
    layout, tile, chan = lax.axis_index("layout"), lax.axis_index("tile"), lax.axis_index("chan")
    x, y = lax.div(tile, side), lax.rem(tile, side)
    along, across = jnp.where(chan == 0, x, y), jnp.where(chan == 0, y, x)
    me = tile * chans + chan
    mine = lax.rem(me, QUARTERS)
    far_first = sorted(range(side), key=lambda d: -min(d, side - d))

    def ahead(value, step):
        if step == 0:
            return value
        value = value + step
        return jnp.where(value >= side, value - side, value)

    def place(to_x, to_y, to_chan):
        return (layout, to_x * side + to_y, to_chan)

    def turned_place(to_along, to_across, to_chan):
        return place(
            jnp.where(chan == 0, to_along, to_across), jnp.where(chan == 0, to_across, to_along), to_chan
        )

    def send(src, dst, send_sem, recv_sem, device):
        pltpu.make_async_remote_copy(
            src_ref=src,
            dst_ref=dst,
            send_sem=send_sem,
            recv_sem=recv_sem,
            device_id=device,
            device_id_type=MESH,
        ).start()

    def await_bytes(ref, sem):
        pltpu.make_async_copy(ref, ref, sem).wait()

    loads = [
        pltpu.make_async_copy(src, dst, load.at[k])
        for k, (src, dst) in enumerate(zip(operands, refs[:8], strict=True))
    ]
    for k in (4, 5, 0, 3, 1, 2, 6, 7):
        loads[k].start()

    steps = [d for d in far_first if d != 0]
    barrier = pltpu.get_barrier_semaphore()
    senders = []
    for d in steps:
        senders += [turned_place(ahead(along, d), across, e) for e in range(chans)]
        senders += [turned_place(along, ahead(across, d), chan)]
    senders += [place(x, y, 1 - chan)]
    for device in senders:
        pl.semaphore_signal(barrier, inc=1, device_id=device, device_id_type=MESH)

    for k in range(6):
        loads[k].wait()

    fill_wide = dot(fill[0].astype(F32).astype(BF16), spread[...], 0)
    slot = lax.broadcasted_iota(jnp.int32, (NT, NT * CAP), 1) % CAP
    sample[0] = jnp.where(slot.astype(F32) < fill_wide, weight[0], 0.0) * (1.0 / 65536.0)
    far = lax.broadcasted_iota(jnp.int32, (NT, NT * CAP), 0) >= NT // 2
    for part, position in (
        (1, (code[0] >> 6).astype(F32) + frac_u[0]),
        (2, (code[0] & (TILE - 1)).astype(F32) + frac_v[0]),
    ):
        sample[part] = jnp.where(far, TILE - position, position)

    lower = lax.broadcasted_iota(jnp.int32, (1, LANES), 1) < LANES // 2

    @pl.loop(0, side)
    def _(to_x):
        for near_y in range(side // 2):
            p = to_x * (side // 2) + near_y
            for part in range(3):
                near = sample[part, pl.ds(p, 1), :]
                away = sample[part, pl.ds(NT - 1 - p, 1), :]
                for q in range(QUARTERS):
                    a = near[:, (q // 2) * LANES : (q // 2 + 1) * LANES]
                    b = away[:, (1 - q // 2) * LANES : (2 - q // 2) * LANES]
                    if q % 2 == 0:
                        row = jnp.where(lower, a, b)
                    else:
                        row = pltpu.roll(jnp.where(lower, b, a), LANES // 2, 1)
                    to_y, to_chan = 2 * near_y + q // 2, q % 2
                    where = to_x * side + to_y if to_chan == 0 else tiles + to_y * side + to_x
                    packed[where, pl.ds(part, 1), :] = row

    pl.semaphore_wait(barrier, len(senders))

    def strand(start):
        return packed.at[pl.ds(start * side, side)]

    for d in steps:
        to_x, to_y = ahead(x, d), ahead(y, d)
        send(strand(to_x), middle.at[:, x * chans + chan], send_1, recv_1, place(to_x, y, 0))
        send(strand(side + to_y), middle.at[:, y * chans + chan], send_1, recv_1, place(x, to_y, 1))
    send(
        strand(jnp.where(chan == 0, side + y, x)),
        middle.at[:, across * chans + chan],
        send_1,
        recv_1,
        place(x, y, 1 - chan),
    )
    middle[:, along * chans + chan] = packed[pl.ds((chan * side + along) * side, side)]
    await_bytes(packed.at[pl.ds(0, (2 * side - 1) * side)], recv_1)
    half_side = side // 2
    own_half = lax.div(across, half_side)
    for d in steps:
        to = ahead(across, d)
        send(middle.at[to], landed.at[across], send_2, recv_2.at[own_half], turned_place(along, to, chan))
    landed[across] = middle[across]

    cell = lax.broadcasted_iota(jnp.int32, (TILE, count), 0).astype(F32)
    direct = lax.broadcasted_iota(jnp.int32, (1, count), 1) < count // 2

    def taper(row):
        distance = cell - row
        inner = jnp.maximum(16.0 - distance * distance, 0.0)
        return inner * inner

    def one_tile(chunk, k):
        def row_of(part, slot):
            own = sorted_[chunk, part, pl.ds(CAP * k + slot, 1)]
            mirrored = sorted_[chunk, part, pl.ds(NT * CAP // 2 - CAP - CAP * k + slot, 1)]
            return jnp.where(direct, own, mirrored)

        total = jnp.zeros((2 * TILE, 2 * TILE), F32)
        for pair in range(CAP // 2):
            lefts, rights = [], []
            for slot in (2 * pair, 2 * pair + 1):
                u_high, u_low = split(taper(row_of(1, slot)) * row_of(0, slot))
                v_high, v_low = split(taper(row_of(2, slot)))
                lefts.append(jnp.concatenate([u_high, u_low], axis=0))
                rights.append(jnp.concatenate([v_high, v_low], axis=0))
            total += dot(jnp.concatenate(lefts, axis=1), jnp.concatenate(rights, axis=1), 1)
        return total[:TILE] + total[TILE:]

    def two_tiles(chunk, pair):
        first, second = one_tile(chunk, 2 * pair), one_tile(chunk, 2 * pair + 1)
        first = first + pltpu.roll(first, TILE, 1)
        second = second + pltpu.roll(second, TILE, 1)
        return jnp.where(upper_half, second, first)

    def take_half(chunk, half):
        for here, blocks in ((own_half == half, half_side - 1), (own_half != half, half_side)):

            @pl.when(here)
            def _():
                await_bytes(landed.at[pl.ds(0, blocks)], recv_2.at[half])

        for part in range(3):
            some = landed[half * half_side : (half + 1) * half_side, :, part, :].reshape(count // 2, LANES)
            sorted_[chunk, part] = jnp.concatenate([some, some], axis=0).T

    upper_half = lax.broadcasted_iota(jnp.int32, (TILE, LANES), 1) >= TILE
    strip = BLOCKS // QUARTERS
    others = []
    for hop in (2, 3, 1):
        other = lax.rem(mine + hop, QUARTERS)
        index = me - mine + other
        others.append((other, (layout, lax.div(index, chans), lax.rem(index, chans))))

    def row_range(index):
        return pl.ds(pl.multiple_of(index * ROWS, ROWS), ROWS)

    cuts = (3 * strip // 4, strip)
    take_half(0, 1)
    for pair in range(strip):
        slab[pair] = two_tiles(0, pair)
    take_half(1, 0)
    for pair in range(strip):
        slab[pair] += two_tiles(1, pair)
        if pair + 1 in cuts:
            first = max([0] + [cut for cut in cuts if cut <= pair])
            some = pair + 1 - first
            for other, device in others:
                send(
                    slab.at[pl.ds(first, some), row_range(other), :],
                    rows.at[pl.ds(mine * strip + first, some)],
                    send_x,
                    recv_x,
                    device,
                )

    rows[pl.ds(mine * strip, strip)] = slab[:, row_range(mine), :]
    for k in (6, 7):
        loads[k].wait()
    await_bytes(rows.at[pl.ds(0, BLOCKS - strip)], recv_x)

    waves = real_transform([rows[t] for t in range(BLOCKS)])
    for k in range(BLOCKS):
        re, im = waves[min(k, BLOCKS - k)]
        c, s = row_twist[0, k : k + 1, :], row_twist[1, k : k + 1, :]
        if im is None:
            turned = (re * c, re * s)
        elif k <= BLOCKS // 2:
            turned = (re * c - im * s, re * s + im * c)
        else:
            turned = (re * c + im * s, re * s - im * c)
        for part in range(2):
            upper, rest = split(turned[part])
            high[ROWS * k : ROWS * (k + 1), LANES * part : LANES * (part + 1)] = upper
            low[ROWS * k : ROWS * (k + 1), LANES * part : LANES * (part + 1)] = rest
    groups = BLOCKS * ROWS // LANES
    for lane in range(0, groups, 2):
        where = slice(LANES * lane, LANES * (lane + 2))
        both = table_dot(row_table, high[where], low[where], 1)
        for part in range(2):
            for extra in range(2):
                spectrum[pl.ds(part * groups + lane + extra, count, stride=2 * groups), :] = both[
                    part * LANES : (part + 1) * LANES, extra * LANES : (extra + 1) * LANES
                ]

    each = 2 * groups

    def block(ref, index):
        return ref.at[pl.ds(pl.multiple_of(index * each, each), each), :]

    def send_column(to_x, to_y, same_chip=False):
        for e in range(1 if same_chip else 0, chans):
            to_chan = chan if e == 0 else 1 - chan
            to = (to_x * side + to_y) * chans + to_chan
            send(block(spectrum, to), block(columns, me), send_b, recv_b, place(to_x, to_y, to_chan))

    for dx, dy in far_chips_first(side):
        send_column(ahead(x, dx), ahead(y, dy))
    send_column(x, y, same_chip=True)

    own = pltpu.make_async_copy(block(spectrum, me), block(columns, me), load.at[0])
    own.start()
    own.wait()
    await_bytes(columns.at[pl.ds(0, (count - 1) * each), :], recv_b)
    await_bytes(packed.at[pl.ds(0, (2 * side - 1) * side)], send_1)
    await_bytes(landed.at[pl.ds(0, side - 1)], send_2)
    await_bytes(rows.at[pl.ds(0, BLOCKS - strip)], send_x)
    await_bytes(columns.at[pl.ds(0, (count - 1) * each), :], send_b)


def column_kernel(columns, col_table, col_twist, last_table, out, image, sem):
    count = col_table.shape[1] // 2
    each = columns.shape[0] // count
    groups, wide, tall = each // 2, G // ROWS, LANES // ROWS
    stores = []
    for pair in range(0, groups, 2):
        parts = [
            [columns[pl.ds(part * groups + pair + extra, count, stride=each), :] for part in range(2)]
            for extra in range(2)
        ]
        stacked = jnp.concatenate([jnp.concatenate(part, axis=0) for part in parts], axis=1)
        high, low = split(stacked)
        tops, ends = col_table[: 2 * wide], col_table[2 * wide :]
        real, imag = (
            table_dot(jnp.concatenate([tops[rows], ends[rows]], axis=0), high, low, 0)
            for rows in (slice(0, wide), slice(wide, 2 * wide))
        )
        c, s = col_twist[0], col_twist[1]
        for extra in range(2):
            lane = pair + extra
            re = real[:, extra * LANES : (extra + 1) * LANES]
            im = imag[:, extra * LANES : (extra + 1) * LANES]
            turned = jnp.concatenate([re * c - im * s, re * s + im * c], axis=1)
            high_turned, low_turned = split(turned)
            both = dot(last_table[...], high_turned, 1)
            half = last_table.shape[0] // 2
            last = both[:half] + both[half:] + dot(last_table[:half], low_turned, 1)
            for l2 in range(ROWS):
                image[tall * lane : tall * (lane + 1), wide * l2 : wide * (l2 + 1)] = last[tall * l2 : tall * (l2 + 1)]
            here = pl.ds(tall * lane, tall)
            stores.append(pltpu.make_async_copy(image.at[here, :], out.at[here, :], sem.at[lane]))
            stores[-1].start()
    for store in stores:
        store.wait()


def body(*inputs):
    tiles, chans = lax.axis_size("tile"), lax.axis_size("chan")
    count, side = tiles * chans, math.isqrt(tiles)
    constants = [jnp.asarray(table) for table in tables(count)]
    operands = [pltpu.with_memory_space_constraint(v, pltpu.HBM) for v in [*inputs, *constants[:3]]]
    columns = pl.pallas_call(
        functools.partial(kernel, tiles, chans),
        out_shape=jax.ShapeDtypeStruct((count * 8, LANES), F32),
        in_specs=[pl.BlockSpec(memory_space=pltpu.HBM)] * len(operands),
        out_specs=pl.BlockSpec(memory_space=pl.ANY),
        scratch_shapes=[pltpu.VMEM(operand.shape, operand.dtype) for operand in operands]
        + [
            pltpu.VMEM((3, NT, NT * CAP), F32),
            pltpu.VMEM((count, 3, LANES), F32),
            pltpu.VMEM((side, side * chans, 3, LANES), F32),
            pltpu.VMEM((side, side * chans, 3, LANES), F32),
            pltpu.VMEM((2, 3, LANES, count), F32),
            pltpu.VMEM((BLOCKS // QUARTERS, TILE, LANES), F32),
            pltpu.VMEM((BLOCKS, ROWS, LANES), F32),
            pltpu.VMEM((BLOCKS * ROWS, 2 * LANES), BF16),
            pltpu.VMEM((BLOCKS * ROWS, 2 * LANES), BF16),
            pltpu.VMEM((count * 8, LANES), F32),
            pltpu.SemaphoreType.DMA((len(operands),)),
        ]
        + [pltpu.SemaphoreType.DMA((2,)) if k == 3 else pltpu.SemaphoreType.DMA for k in range(8)],
        compiler_params=pltpu.CompilerParams(
            collective_id=0, has_side_effects=True, vmem_limit_bytes=VMEM_LIMIT
        ),
    )(*operands)
    return pl.pallas_call(
        column_kernel,
        out_shape=jax.ShapeDtypeStruct((OUT_ROWS, G), F32),
        in_specs=[pl.BlockSpec(memory_space=pltpu.VMEM)] * 4,
        out_specs=pl.BlockSpec(memory_space=pl.ANY),
        scratch_shapes=[
            pltpu.VMEM((OUT_ROWS, G), F32),
            pltpu.SemaphoreType.DMA((BLOCKS * ROWS // LANES,)),
        ],
        compiler_params=pltpu.CompilerParams(vmem_limit_bytes=VMEM_LIMIT),
    )(columns, *constants[3:])


def solution(mesh):
    spec = P(("layout", "tile", "chan"), None, None)
    return jax.shard_map(
        body,
        mesh=mesh,
        in_specs=(spec,) * 5,
        out_specs=P(("layout", "tile", "chan"), None),
        check_vma=False,
    )
```

```python
import functools
import math

import jax
import jax.numpy as jnp
import numpy as np
from jax import lax
from jax.experimental import pallas as pl
from jax.experimental.pallas import tpu as pltpu
from jax.sharding import PartitionSpec as P

G = 4096
TILE = 64
CAP = 4
NT = 64
LANES = 128
QUARTERS = 4
ROWS = TILE // QUARTERS
BLOCKS = G // LANES
OUT_ROWS = 32
MESH = pl.DeviceIdType.MESH
VMEM_LIMIT = 16 * 2**20
F32 = jnp.float32
BF16 = jnp.bfloat16


def two_parts(table):
    table = np.asarray(table, np.float32)
    high = table.astype(BF16)
    low = (table - high.astype(np.float32)).astype(BF16)
    return np.concatenate([high, low], axis=0)


@functools.lru_cache
def tables(devices):
    spread = (np.arange(NT)[:, None] == np.arange(NT * CAP)[None, :] // CAP).astype(BF16)
    turn = 2.0 * np.pi * np.outer(np.arange(LANES), np.arange(LANES)) / LANES
    cos, sin = np.cos(turn), np.sin(turn)
    row_table = two_parts(np.block([[cos, -sin], [sin, cos]]))
    turn = 2.0 * np.pi * np.outer(np.arange(BLOCKS), np.arange(LANES)) / G
    row_twist = np.stack([np.cos(turn), np.sin(turn)]).astype(np.float32)
    wide = G // ROWS
    turn = 2.0 * np.pi * np.outer(np.arange(wide), np.arange(devices)) / wide
    cos, sin = np.cos(turn), np.sin(turn)
    col_table = two_parts(np.block([[cos, -sin], [sin, cos]]))
    turn = 2.0 * np.pi * np.outer(np.arange(wide), np.arange(LANES) % ROWS) / G
    col_twist = np.stack([np.cos(turn), np.sin(turn)]).astype(np.float32)
    group = LANES // ROWS
    out_index = np.arange(ROWS * group)
    lane = np.arange(LANES)
    same = (out_index[:, None] % group == lane[None, :] // ROWS) / math.sqrt(devices * NT * NT * CAP)
    turn = 2.0 * np.pi * np.outer(out_index // group, lane % ROWS) / ROWS
    last_table = two_parts(np.concatenate([same * np.cos(turn), -same * np.sin(turn)], axis=1))
    return spread, row_table, row_twist, col_table, col_twist, last_table


def split(value):
    high = value.astype(BF16)
    return high, (value - high.astype(F32)).astype(BF16)


def dot(left, right, right_dim):
    return lax.dot_general(left, right, (((1,), (right_dim,)), ((), ())), preferred_element_type=F32)


def table_dot(table, high, low, right_dim):
    half = table.shape[0] // 2
    return dot(table[:half], high, right_dim) + dot(table[half:], high, right_dim) + dot(table[:half], low, right_dim)


def times(value, real, imag):
    v_re, v_im = value
    if abs(imag) < 1e-12:
        if abs(real - 1.0) < 1e-12:
            return value
        return v_re * real, None if v_im is None else v_im * real
    if v_im is None:
        return (None if abs(real) < 1e-12 else v_re * real), v_re * imag
    if abs(real) < 1e-12:
        return -v_im * imag, v_re * imag
    return v_re * real - v_im * imag, v_re * imag + v_im * real


def plus(a, b, sign):
    if b is None:
        return a
    if a is None:
        return b if sign > 0 else -b
    return a + b if sign > 0 else a - b


def real_transform(values):
    count = len(values)
    if count == 1:
        return [(values[0], None)]
    if count == 2:
        return [(values[0] + values[1], None), (values[0] - values[1], None)]
    even, odd = real_transform(values[0::2]), real_transform(values[1::2])
    out = [None] * (count // 2 + 1)
    for k in range(count // 4 + 1):
        turn = 2.0 * math.pi * k / count
        turned = times(odd[k], math.cos(turn), math.sin(turn))
        out[k] = (plus(even[k][0], turned[0], 1), plus(even[k][1], turned[1], 1))
        far_im = plus(even[k][1], turned[1], -1)
        out[count // 2 - k] = (plus(even[k][0], turned[0], -1), None if far_im is None else -far_im)
    return out


def far_chips_first(side):
    half = side // 2
    ties = [step for j in range(side) for step in ([(half, j), (j, half)] if j != half else [(half, half)])]
    quarter = [(a, b) for a in range(half - 1, 0, -1) for b in range(half - 1, -1, -1)]
    quarter.sort(key=lambda step: -sum(step))
    turned = [step for a, b in quarter for step in ((a, b), (-b, a), (-a, -b), (b, -a))]
    return [(dx % side, dy % side) for dx, dy in ties + turned]


def kernel(tiles, chans, *refs):
    operands, columns, refs = refs[:8], refs[8], refs[9:]
    weight, frac_u, frac_v, code, fill, spread, row_table, row_twist = refs[:8]
    sample, packed, middle, landed, sorted_, slab, rows, high, low, spectrum = refs[8:18]
    load, send_1, recv_1, send_2, recv_2, send_x, recv_x, send_b, recv_b = refs[18:]
    side = math.isqrt(tiles)
    count = tiles * chans
    layout, tile, chan = lax.axis_index("layout"), lax.axis_index("tile"), lax.axis_index("chan")
    x, y = lax.div(tile, side), lax.rem(tile, side)
    along, across = jnp.where(chan == 0, x, y), jnp.where(chan == 0, y, x)
    me = tile * chans + chan
    mine = lax.rem(me, QUARTERS)
    far_first = sorted(range(side), key=lambda d: -min(d, side - d))

    def ahead(value, step):
        if step == 0:
            return value
        value = value + step
        return jnp.where(value >= side, value - side, value)

    def place(to_x, to_y, to_chan):
        return (layout, to_x * side + to_y, to_chan)

    def turned_place(to_along, to_across, to_chan):
        return place(
            jnp.where(chan == 0, to_along, to_across), jnp.where(chan == 0, to_across, to_along), to_chan
        )

    def send(src, dst, send_sem, recv_sem, device):
        pltpu.make_async_remote_copy(
            src_ref=src,
            dst_ref=dst,
            send_sem=send_sem,
            recv_sem=recv_sem,
            device_id=device,
            device_id_type=MESH,
        ).start()

    def await_bytes(ref, sem):
        pltpu.make_async_copy(ref, ref, sem).wait()

    loads = [
        pltpu.make_async_copy(src, dst, load.at[k])
        for k, (src, dst) in enumerate(zip(operands, refs[:8], strict=True))
    ]
    for k in (4, 5, 0, 3, 1, 2, 6, 7):
        loads[k].start()

    steps = [d for d in far_first if d != 0]
    barrier = pltpu.get_barrier_semaphore()
    senders = []
    for d in steps:
        senders += [turned_place(ahead(along, d), across, e) for e in range(chans)]
        senders += [turned_place(along, ahead(across, d), chan)]
    senders += [place(x, y, 1 - chan)]
    for device in senders:
        pl.semaphore_signal(barrier, inc=1, device_id=device, device_id_type=MESH)

    for k in range(6):
        loads[k].wait()

    fill_wide = dot(fill[0].astype(F32).astype(BF16), spread[...], 0)
    slot = lax.broadcasted_iota(jnp.int32, (NT, NT * CAP), 1) % CAP
    sample[0] = jnp.where(slot.astype(F32) < fill_wide, weight[0], 0.0) * (1.0 / 65536.0)
    far = lax.broadcasted_iota(jnp.int32, (NT, NT * CAP), 0) >= NT // 2
    for part, position in (
        (1, (code[0] >> 6).astype(F32) + frac_u[0]),
        (2, (code[0] & (TILE - 1)).astype(F32) + frac_v[0]),
    ):
        sample[part] = jnp.where(far, TILE - position, position)

    lower = lax.broadcasted_iota(jnp.int32, (1, LANES), 1) < LANES // 2

    @pl.loop(0, side)
    def _(to_x):
        for near_y in range(side // 2):
            p = to_x * (side // 2) + near_y
            for part in range(3):
                near = sample[part, pl.ds(p, 1), :]
                away = sample[part, pl.ds(NT - 1 - p, 1), :]
                for q in range(QUARTERS):
                    a = near[:, (q // 2) * LANES : (q // 2 + 1) * LANES]
                    b = away[:, (1 - q // 2) * LANES : (2 - q // 2) * LANES]
                    if q % 2 == 0:
                        row = jnp.where(lower, a, b)
                    else:
                        row = pltpu.roll(jnp.where(lower, b, a), LANES // 2, 1)
                    to_y, to_chan = 2 * near_y + q // 2, q % 2
                    where = to_x * side + to_y if to_chan == 0 else tiles + to_y * side + to_x
                    packed[where, pl.ds(part, 1), :] = row

    pl.semaphore_wait(barrier, len(senders))

    def strand(start):
        return packed.at[pl.ds(start * side, side)]

    for d in steps:
        to_x, to_y = ahead(x, d), ahead(y, d)
        send(strand(to_x), middle.at[:, x * chans + chan], send_1, recv_1, place(to_x, y, 0))
        send(strand(side + to_y), middle.at[:, y * chans + chan], send_1, recv_1, place(x, to_y, 1))
    send(
        strand(jnp.where(chan == 0, side + y, x)),
        middle.at[:, across * chans + chan],
        send_1,
        recv_1,
        place(x, y, 1 - chan),
    )
    middle[:, along * chans + chan] = packed[pl.ds((chan * side + along) * side, side)]
    await_bytes(packed.at[pl.ds(0, (2 * side - 1) * side)], recv_1)
    for d in steps:
        to = ahead(across, d)
        send(middle.at[to], landed.at[across], send_2, recv_2, turned_place(along, to, chan))
    landed[across] = middle[across]
    await_bytes(landed.at[pl.ds(0, side - 1)], recv_2)

    for part in range(3):
        sorted_[part] = landed[:, :, part, :].reshape(count, LANES).T

    cell = lax.broadcasted_iota(jnp.int32, (TILE, count), 0).astype(F32)

    def taper(row, where):
        distance = cell - row[where]
        inner = jnp.maximum(16.0 - distance * distance, 0.0)
        return inner * inner

    def one_tile(k):
        total = jnp.zeros((2 * TILE, 2 * TILE), F32)
        starts = [CAP * k, NT * CAP // 2 - CAP - CAP * k]
        for start in starts:
            for pair in range(CAP // 2):
                lefts, rights = [], []
                for slot in range(2):
                    where = pl.ds(start + 2 * pair + slot, 1)
                    u_high, u_low = split(taper(sorted_.at[1], where) * sorted_[0, where])
                    v_high, v_low = split(taper(sorted_.at[2], where))
                    lefts.append(jnp.concatenate([u_high, u_low], axis=0))
                    rights.append(jnp.concatenate([v_high, v_low], axis=0))
                total += dot(jnp.concatenate(lefts, axis=1), jnp.concatenate(rights, axis=1), 1)
        return total[:TILE] + total[TILE:]

    upper_half = lax.broadcasted_iota(jnp.int32, (TILE, LANES), 1) >= TILE
    strip = BLOCKS // QUARTERS
    others = []
    for hop in (2, 3, 1):
        other = lax.rem(mine + hop, QUARTERS)
        index = me - mine + other
        others.append((other, (layout, lax.div(index, chans), lax.rem(index, chans))))

    def row_range(index):
        return pl.ds(pl.multiple_of(index * ROWS, ROWS), ROWS)

    cuts = (3 * strip // 4, strip)
    for pair in range(strip):
        first, second = one_tile(2 * pair), one_tile(2 * pair + 1)
        first = first + pltpu.roll(first, TILE, 1)
        second = second + pltpu.roll(second, TILE, 1)
        slab[pair] = jnp.where(upper_half, second, first)
        if pair + 1 in cuts:
            first = max([0] + [cut for cut in cuts if cut <= pair])
            some = pair + 1 - first
            for other, device in others:
                send(
                    slab.at[pl.ds(first, some), row_range(other), :],
                    rows.at[pl.ds(mine * strip + first, some)],
                    send_x,
                    recv_x,
                    device,
                )

    rows[pl.ds(mine * strip, strip)] = slab[:, row_range(mine), :]
    for k in (6, 7):
        loads[k].wait()
    await_bytes(rows.at[pl.ds(0, BLOCKS - strip)], recv_x)

    waves = real_transform([rows[t] for t in range(BLOCKS)])
    for k in range(BLOCKS):
        re, im = waves[min(k, BLOCKS - k)]
        c, s = row_twist[0, k : k + 1, :], row_twist[1, k : k + 1, :]
        if im is None:
            turned = (re * c, re * s)
        elif k <= BLOCKS // 2:
            turned = (re * c - im * s, re * s + im * c)
        else:
            turned = (re * c + im * s, re * s - im * c)
        for part in range(2):
            upper, rest = split(turned[part])
            high[ROWS * k : ROWS * (k + 1), LANES * part : LANES * (part + 1)] = upper
            low[ROWS * k : ROWS * (k + 1), LANES * part : LANES * (part + 1)] = rest
    groups = BLOCKS * ROWS // LANES
    for lane in range(0, groups, 2):
        where = slice(LANES * lane, LANES * (lane + 2))
        both = table_dot(row_table, high[where], low[where], 1)
        for part in range(2):
            for extra in range(2):
                spectrum[pl.ds(part * groups + lane + extra, count, stride=2 * groups), :] = both[
                    part * LANES : (part + 1) * LANES, extra * LANES : (extra + 1) * LANES
                ]

    each = 2 * groups

    def block(ref, index):
        return ref.at[pl.ds(pl.multiple_of(index * each, each), each), :]

    def send_column(to_x, to_y, same_chip=False):
        for e in range(1 if same_chip else 0, chans):
            to_chan = chan if e == 0 else 1 - chan
            to = (to_x * side + to_y) * chans + to_chan
            send(block(spectrum, to), block(columns, me), send_b, recv_b, place(to_x, to_y, to_chan))

    for dx, dy in far_chips_first(side):
        send_column(ahead(x, dx), ahead(y, dy))
    send_column(x, y, same_chip=True)

    own = pltpu.make_async_copy(block(spectrum, me), block(columns, me), load.at[0])
    own.start()
    own.wait()
    await_bytes(columns.at[pl.ds(0, (count - 1) * each), :], recv_b)
    await_bytes(packed.at[pl.ds(0, (2 * side - 1) * side)], send_1)
    await_bytes(landed.at[pl.ds(0, side - 1)], send_2)
    await_bytes(rows.at[pl.ds(0, BLOCKS - strip)], send_x)
    await_bytes(columns.at[pl.ds(0, (count - 1) * each), :], send_b)


def column_kernel(columns, col_table, col_twist, last_table, out, image, sem):
    count = col_table.shape[1] // 2
    each = columns.shape[0] // count
    groups, wide, tall = each // 2, G // ROWS, LANES // ROWS
    stores = []
    for pair in range(0, groups, 2):
        parts = [
            [columns[pl.ds(part * groups + pair + extra, count, stride=each), :] for part in range(2)]
            for extra in range(2)
        ]
        stacked = jnp.concatenate([jnp.concatenate(part, axis=0) for part in parts], axis=1)
        high, low = split(stacked)
        tops, ends = col_table[: 2 * wide], col_table[2 * wide :]
        real, imag = (
            table_dot(jnp.concatenate([tops[rows], ends[rows]], axis=0), high, low, 0)
            for rows in (slice(0, wide), slice(wide, 2 * wide))
        )
        c, s = col_twist[0], col_twist[1]
        for extra in range(2):
            lane = pair + extra
            re = real[:, extra * LANES : (extra + 1) * LANES]
            im = imag[:, extra * LANES : (extra + 1) * LANES]
            turned = jnp.concatenate([re * c - im * s, re * s + im * c], axis=1)
            high_turned, low_turned = split(turned)
            both = dot(last_table[...], high_turned, 1)
            half = last_table.shape[0] // 2
            last = both[:half] + both[half:] + dot(last_table[:half], low_turned, 1)
            for l2 in range(ROWS):
                image[tall * lane : tall * (lane + 1), wide * l2 : wide * (l2 + 1)] = last[tall * l2 : tall * (l2 + 1)]
            here = pl.ds(tall * lane, tall)
            stores.append(pltpu.make_async_copy(image.at[here, :], out.at[here, :], sem.at[lane]))
            stores[-1].start()
    for store in stores:
        store.wait()


def body(*inputs):
    tiles, chans = lax.axis_size("tile"), lax.axis_size("chan")
    count, side = tiles * chans, math.isqrt(tiles)
    constants = [jnp.asarray(table) for table in tables(count)]
    operands = [pltpu.with_memory_space_constraint(v, pltpu.HBM) for v in [*inputs, *constants[:3]]]
    columns = pl.pallas_call(
        functools.partial(kernel, tiles, chans),
        out_shape=jax.ShapeDtypeStruct((count * 8, LANES), F32),
        in_specs=[pl.BlockSpec(memory_space=pltpu.HBM)] * len(operands),
        out_specs=pl.BlockSpec(memory_space=pl.ANY),
        scratch_shapes=[pltpu.VMEM(operand.shape, operand.dtype) for operand in operands]
        + [
            pltpu.VMEM((3, NT, NT * CAP), F32),
            pltpu.VMEM((count, 3, LANES), F32),
            pltpu.VMEM((side, side * chans, 3, LANES), F32),
            pltpu.VMEM((side, side * chans, 3, LANES), F32),
            pltpu.VMEM((3, LANES, count), F32),
            pltpu.VMEM((BLOCKS // QUARTERS, TILE, LANES), F32),
            pltpu.VMEM((BLOCKS, ROWS, LANES), F32),
            pltpu.VMEM((BLOCKS * ROWS, 2 * LANES), BF16),
            pltpu.VMEM((BLOCKS * ROWS, 2 * LANES), BF16),
            pltpu.VMEM((count * 8, LANES), F32),
            pltpu.SemaphoreType.DMA((len(operands),)),
        ]
        + [pltpu.SemaphoreType.DMA] * 8,
        compiler_params=pltpu.CompilerParams(
            collective_id=0, has_side_effects=True, vmem_limit_bytes=VMEM_LIMIT
        ),
    )(*operands)
    return pl.pallas_call(
        column_kernel,
        out_shape=jax.ShapeDtypeStruct((OUT_ROWS, G), F32),
        in_specs=[pl.BlockSpec(memory_space=pltpu.VMEM)] * 4,
        out_specs=pl.BlockSpec(memory_space=pl.ANY),
        scratch_shapes=[
            pltpu.VMEM((OUT_ROWS, G), F32),
            pltpu.SemaphoreType.DMA((BLOCKS * ROWS // LANES,)),
        ],
        compiler_params=pltpu.CompilerParams(vmem_limit_bytes=VMEM_LIMIT),
    )(columns, *constants[3:])


def solution(mesh):
    spec = P(("layout", "tile", "chan"), None, None)
    return jax.shard_map(
        body,
        mesh=mesh,
        in_specs=(spec,) * 5,
        out_specs=P(("layout", "tile", "chan"), None),
        check_vma=False,
    )
```

```python
import functools
import math

import jax
import jax.numpy as jnp
import numpy as np
from jax import lax
from jax.experimental import pallas as pl
from jax.experimental.pallas import tpu as pltpu
from jax.sharding import PartitionSpec as P

G = 4096
TILE = 64
CAP = 4
NT = 64
LANES = 128
QUARTERS = 4
ROWS = TILE // QUARTERS
BLOCKS = G // LANES
OUT_ROWS = 32
MESH = pl.DeviceIdType.MESH
VMEM_LIMIT = 16 * 2**20
F32 = jnp.float32
BF16 = jnp.bfloat16


def two_parts(table):
    table = np.asarray(table, np.float32)
    high = table.astype(BF16)
    low = (table - high.astype(np.float32)).astype(BF16)
    return np.concatenate([high, low], axis=0)


@functools.lru_cache
def tables(devices):
    spread = (np.arange(NT)[:, None] == np.arange(NT * CAP)[None, :] // CAP).astype(BF16)
    turn = 2.0 * np.pi * np.outer(np.arange(LANES), np.arange(LANES)) / LANES
    cos, sin = np.cos(turn), np.sin(turn)
    row_table = two_parts(np.block([[cos, -sin], [sin, cos]]))
    turn = 2.0 * np.pi * np.outer(np.arange(BLOCKS), np.arange(LANES)) / G
    row_twist = np.stack([np.cos(turn), np.sin(turn)]).astype(np.float32)
    wide = G // ROWS
    turn = 2.0 * np.pi * np.outer(np.arange(wide), np.arange(devices)) / wide
    cos, sin = np.cos(turn), np.sin(turn)
    col_table = two_parts(np.block([[cos, -sin], [sin, cos]]))
    turn = 2.0 * np.pi * np.outer(np.arange(wide), np.arange(LANES) % ROWS) / G
    col_twist = np.stack([np.cos(turn), np.sin(turn)]).astype(np.float32)
    group = LANES // ROWS
    out_index = np.arange(ROWS * group)
    lane = np.arange(LANES)
    same = (out_index[:, None] % group == lane[None, :] // ROWS) / math.sqrt(devices * NT * NT * CAP)
    turn = 2.0 * np.pi * np.outer(out_index // group, lane % ROWS) / ROWS
    last_table = two_parts(np.concatenate([same * np.cos(turn), -same * np.sin(turn)], axis=1))
    return spread, row_table, row_twist, col_table, col_twist, last_table


def split(value):
    high = value.astype(BF16)
    return high, (value - high.astype(F32)).astype(BF16)


def dot(left, right, right_dim):
    return lax.dot_general(left, right, (((1,), (right_dim,)), ((), ())), preferred_element_type=F32)


def table_dot(table, high, low, right_dim):
    half = table.shape[0] // 2
    return dot(table[:half], high, right_dim) + dot(table[half:], high, right_dim) + dot(table[:half], low, right_dim)


def times(value, real, imag):
    v_re, v_im = value
    if abs(imag) < 1e-12:
        if abs(real - 1.0) < 1e-12:
            return value
        return v_re * real, None if v_im is None else v_im * real
    if v_im is None:
        return (None if abs(real) < 1e-12 else v_re * real), v_re * imag
    if abs(real) < 1e-12:
        return -v_im * imag, v_re * imag
    return v_re * real - v_im * imag, v_re * imag + v_im * real


def plus(a, b, sign):
    if b is None:
        return a
    if a is None:
        return b if sign > 0 else -b
    return a + b if sign > 0 else a - b


def real_transform(values):
    count = len(values)
    if count == 1:
        return [(values[0], None)]
    if count == 2:
        return [(values[0] + values[1], None), (values[0] - values[1], None)]
    even, odd = real_transform(values[0::2]), real_transform(values[1::2])
    out = [None] * (count // 2 + 1)
    for k in range(count // 4 + 1):
        turn = 2.0 * math.pi * k / count
        turned = times(odd[k], math.cos(turn), math.sin(turn))
        out[k] = (plus(even[k][0], turned[0], 1), plus(even[k][1], turned[1], 1))
        far_im = plus(even[k][1], turned[1], -1)
        out[count // 2 - k] = (plus(even[k][0], turned[0], -1), None if far_im is None else -far_im)
    return out


def far_chips_first(side):
    half = side // 2
    ties = [step for j in range(side) for step in ([(half, j), (j, half)] if j != half else [(half, half)])]
    quarter = [(a, b) for a in range(half - 1, 0, -1) for b in range(half - 1, -1, -1)]
    quarter.sort(key=lambda step: -sum(step))
    turned = [step for a, b in quarter for step in ((a, b), (-b, a), (-a, -b), (b, -a))]
    return [(dx % side, dy % side) for dx, dy in ties + turned]


def kernel(tiles, chans, *refs):
    operands, columns, refs = refs[:8], refs[8], refs[9:]
    weight, frac_u, frac_v, code, fill, spread, row_table, row_twist = refs[:8]
    sample, packed, middle, landed, sorted_, slab, rows, high, low, spectrum = refs[8:18]
    load, send_1, recv_1, send_2, recv_2, send_x, recv_x, send_b, recv_b = refs[18:]
    side = math.isqrt(tiles)
    count = tiles * chans
    layout, tile, chan = lax.axis_index("layout"), lax.axis_index("tile"), lax.axis_index("chan")
    x, y = lax.div(tile, side), lax.rem(tile, side)
    along, across = jnp.where(chan == 0, x, y), jnp.where(chan == 0, y, x)
    me = tile * chans + chan
    mine = lax.rem(me, QUARTERS)
    far_first = sorted(range(side), key=lambda d: -min(d, side - d))

    def ahead(value, step):
        if step == 0:
            return value
        value = value + step
        return jnp.where(value >= side, value - side, value)

    def place(to_x, to_y, to_chan):
        return (layout, to_x * side + to_y, to_chan)

    def turned_place(to_along, to_across, to_chan):
        return place(
            jnp.where(chan == 0, to_along, to_across), jnp.where(chan == 0, to_across, to_along), to_chan
        )

    def send(src, dst, send_sem, recv_sem, device):
        pltpu.make_async_remote_copy(
            src_ref=src,
            dst_ref=dst,
            send_sem=send_sem,
            recv_sem=recv_sem,
            device_id=device,
            device_id_type=MESH,
        ).start()

    def await_bytes(ref, sem):
        pltpu.make_async_copy(ref, ref, sem).wait()

    loads = [
        pltpu.make_async_copy(src, dst, load.at[k])
        for k, (src, dst) in enumerate(zip(operands, refs[:8], strict=True))
    ]
    for k in (4, 5, 0, 3, 1, 2, 6, 7):
        loads[k].start()

    steps = [d for d in far_first if d != 0]
    barrier = pltpu.get_barrier_semaphore()
    senders = [turned_place(ahead(along, d), across, e) for d in steps for e in range(chans)]
    senders += [turned_place(along, ahead(across, d), chan) for d in steps]
    senders += [place(x, y, 1 - chan)]
    for device in senders:
        pl.semaphore_signal(barrier, inc=1, device_id=device, device_id_type=MESH)

    for k in range(6):
        loads[k].wait()

    fill_wide = dot(fill[0].astype(F32).astype(BF16), spread[...], 0)
    slot = lax.broadcasted_iota(jnp.int32, (NT, NT * CAP), 1) % CAP
    sample[0] = jnp.where(slot.astype(F32) < fill_wide, weight[0], 0.0) * (1.0 / 65536.0)
    far = lax.broadcasted_iota(jnp.int32, (NT, NT * CAP), 0) >= NT // 2
    for part, position in (
        (1, (code[0] >> 6).astype(F32) + frac_u[0]),
        (2, (code[0] & (TILE - 1)).astype(F32) + frac_v[0]),
    ):
        sample[part] = jnp.where(far, TILE - position, position)

    lower = lax.broadcasted_iota(jnp.int32, (1, LANES), 1) < LANES // 2

    @pl.loop(0, side)
    def _(to_x):
        for near_y in range(side // 2):
            p = to_x * (side // 2) + near_y
            for part in range(3):
                near = sample[part, pl.ds(p, 1), :]
                away = sample[part, pl.ds(NT - 1 - p, 1), :]
                for q in range(QUARTERS):
                    a = near[:, (q // 2) * LANES : (q // 2 + 1) * LANES]
                    b = away[:, (1 - q // 2) * LANES : (2 - q // 2) * LANES]
                    if q % 2 == 0:
                        row = jnp.where(lower, a, b)
                    else:
                        row = pltpu.roll(jnp.where(lower, b, a), LANES // 2, 1)
                    to_y, to_chan = 2 * near_y + q // 2, q % 2
                    where = to_x * side + to_y if to_chan == 0 else tiles + to_y * side + to_x
                    packed[where, pl.ds(part, 1), :] = row

    pl.semaphore_wait(barrier, len(senders))

    def strand(start):
        return packed.at[pl.ds(start * side, side)]

    for d in steps:
        to_x, to_y = ahead(x, d), ahead(y, d)
        send(strand(to_x), middle.at[:, x * chans + chan], send_1, recv_1, place(to_x, y, 0))
        send(strand(side + to_y), middle.at[:, y * chans + chan], send_1, recv_1, place(x, to_y, 1))
    send(
        strand(jnp.where(chan == 0, side + y, x)),
        middle.at[:, across * chans + chan],
        send_1,
        recv_1,
        place(x, y, 1 - chan),
    )
    middle[:, along * chans + chan] = packed[pl.ds((chan * side + along) * side, side)]
    await_bytes(packed.at[pl.ds(0, (2 * side - 1) * side)], recv_1)
    for d in steps:
        to = ahead(across, d)
        send(middle.at[to], landed.at[across], send_2, recv_2, turned_place(along, to, chan))
    landed[across] = middle[across]
    await_bytes(landed.at[pl.ds(0, side - 1)], recv_2)

    for part in range(3):
        sorted_[part] = landed[:, :, part, :].reshape(count, LANES).T

    cell = lax.broadcasted_iota(jnp.int32, (TILE, count), 0).astype(F32)

    def taper(row, where):
        distance = cell - row[where]
        inner = jnp.maximum(16.0 - distance * distance, 0.0)
        return inner * inner

    def one_tile(k):
        total = jnp.zeros((2 * TILE, 2 * TILE), F32)
        starts = [CAP * k, NT * CAP // 2 - CAP - CAP * k]
        for start in starts:
            for pair in range(CAP // 2):
                lefts, rights = [], []
                for slot in range(2):
                    where = pl.ds(start + 2 * pair + slot, 1)
                    u_high, u_low = split(taper(sorted_.at[1], where) * sorted_[0, where])
                    v_high, v_low = split(taper(sorted_.at[2], where))
                    lefts.append(jnp.concatenate([u_high, u_low], axis=0))
                    rights.append(jnp.concatenate([v_high, v_low], axis=0))
                total += dot(jnp.concatenate(lefts, axis=1), jnp.concatenate(rights, axis=1), 1)
        return total[:TILE] + total[TILE:]

    upper_half = lax.broadcasted_iota(jnp.int32, (TILE, LANES), 1) >= TILE
    strip = BLOCKS // QUARTERS
    others = []
    for hop in (2, 3, 1):
        other = lax.rem(mine + hop, QUARTERS)
        index = me - mine + other
        others.append((other, (layout, lax.div(index, chans), lax.rem(index, chans))))

    def row_range(index):
        return pl.ds(pl.multiple_of(index * ROWS, ROWS), ROWS)

    cuts = (3 * strip // 4, strip)
    for pair in range(strip):
        first, second = one_tile(2 * pair), one_tile(2 * pair + 1)
        first = first + pltpu.roll(first, TILE, 1)
        second = second + pltpu.roll(second, TILE, 1)
        slab[pair] = jnp.where(upper_half, second, first)
        if pair + 1 in cuts:
            first = max([0] + [cut for cut in cuts if cut <= pair])
            some = pair + 1 - first
            for other, device in others:
                send(
                    slab.at[pl.ds(first, some), row_range(other), :],
                    rows.at[pl.ds(mine * strip + first, some)],
                    send_x,
                    recv_x,
                    device,
                )

    rows[pl.ds(mine * strip, strip)] = slab[:, row_range(mine), :]
    for k in (6, 7):
        loads[k].wait()
    await_bytes(rows.at[pl.ds(0, BLOCKS - strip)], recv_x)

    waves = real_transform([rows[t] for t in range(BLOCKS)])
    for k in range(BLOCKS):
        re, im = waves[min(k, BLOCKS - k)]
        c, s = row_twist[0, k : k + 1, :], row_twist[1, k : k + 1, :]
        if im is None:
            turned = (re * c, re * s)
        elif k <= BLOCKS // 2:
            turned = (re * c - im * s, re * s + im * c)
        else:
            turned = (re * c + im * s, re * s - im * c)
        for part in range(2):
            upper, rest = split(turned[part])
            high[ROWS * k : ROWS * (k + 1), LANES * part : LANES * (part + 1)] = upper
            low[ROWS * k : ROWS * (k + 1), LANES * part : LANES * (part + 1)] = rest
    groups = BLOCKS * ROWS // LANES
    for lane in range(0, groups, 2):
        where = slice(LANES * lane, LANES * (lane + 2))
        both = table_dot(row_table, high[where], low[where], 1)
        for part in range(2):
            for extra in range(2):
                spectrum[pl.ds(part * groups + lane + extra, count, stride=2 * groups), :] = both[
                    part * LANES : (part + 1) * LANES, extra * LANES : (extra + 1) * LANES
                ]

    each = 2 * groups

    def block(ref, index):
        return ref.at[pl.ds(pl.multiple_of(index * each, each), each), :]

    def send_column(to_x, to_y, same_chip=False):
        for e in range(1 if same_chip else 0, chans):
            to_chan = chan if e == 0 else 1 - chan
            to = (to_x * side + to_y) * chans + to_chan
            send(block(spectrum, to), block(columns, me), send_b, recv_b, place(to_x, to_y, to_chan))

    for dx, dy in far_chips_first(side):
        send_column(ahead(x, dx), ahead(y, dy))
    send_column(x, y, same_chip=True)

    own = pltpu.make_async_copy(block(spectrum, me), block(columns, me), load.at[0])
    own.start()
    own.wait()
    await_bytes(columns.at[pl.ds(0, (count - 1) * each), :], recv_b)
    await_bytes(packed.at[pl.ds(0, (2 * side - 1) * side)], send_1)
    await_bytes(landed.at[pl.ds(0, side - 1)], send_2)
    await_bytes(rows.at[pl.ds(0, BLOCKS - strip)], send_x)
    await_bytes(columns.at[pl.ds(0, (count - 1) * each), :], send_b)


def column_kernel(columns, col_table, col_twist, last_table, out, image, sem):
    count = col_table.shape[1] // 2
    each = columns.shape[0] // count
    groups, wide, tall = each // 2, G // ROWS, LANES // ROWS
    stores = []
    for pair in range(0, groups, 2):
        parts = [
            [columns[pl.ds(part * groups + pair + extra, count, stride=each), :] for part in range(2)]
            for extra in range(2)
        ]
        stacked = jnp.concatenate([jnp.concatenate(part, axis=0) for part in parts], axis=1)
        high, low = split(stacked)
        tops, ends = col_table[: 2 * wide], col_table[2 * wide :]
        real, imag = (
            table_dot(jnp.concatenate([tops[rows], ends[rows]], axis=0), high, low, 0)
            for rows in (slice(0, wide), slice(wide, 2 * wide))
        )
        c, s = col_twist[0], col_twist[1]
        for extra in range(2):
            lane = pair + extra
            re = real[:, extra * LANES : (extra + 1) * LANES]
            im = imag[:, extra * LANES : (extra + 1) * LANES]
            turned = jnp.concatenate([re * c - im * s, re * s + im * c], axis=1)
            high_turned, low_turned = split(turned)
            both = dot(last_table[...], high_turned, 1)
            half = last_table.shape[0] // 2
            last = both[:half] + both[half:] + dot(last_table[:half], low_turned, 1)
            for l2 in range(ROWS):
                image[tall * lane : tall * (lane + 1), wide * l2 : wide * (l2 + 1)] = last[tall * l2 : tall * (l2 + 1)]
            here = pl.ds(tall * lane, tall)
            stores.append(pltpu.make_async_copy(image.at[here, :], out.at[here, :], sem.at[lane]))
            stores[-1].start()
    for store in stores:
        store.wait()


def body(*inputs):
    tiles, chans = lax.axis_size("tile"), lax.axis_size("chan")
    count, side = tiles * chans, math.isqrt(tiles)
    constants = [jnp.asarray(table) for table in tables(count)]
    operands = [pltpu.with_memory_space_constraint(v, pltpu.HBM) for v in [*inputs, *constants[:3]]]
    columns = pl.pallas_call(
        functools.partial(kernel, tiles, chans),
        out_shape=jax.ShapeDtypeStruct((count * 8, LANES), F32),
        in_specs=[pl.BlockSpec(memory_space=pltpu.HBM)] * len(operands),
        out_specs=pl.BlockSpec(memory_space=pl.ANY),
        scratch_shapes=[pltpu.VMEM(operand.shape, operand.dtype) for operand in operands]
        + [
            pltpu.VMEM((3, NT, NT * CAP), F32),
            pltpu.VMEM((count, 3, LANES), F32),
            pltpu.VMEM((side, side * chans, 3, LANES), F32),
            pltpu.VMEM((side, side * chans, 3, LANES), F32),
            pltpu.VMEM((3, LANES, count), F32),
            pltpu.VMEM((BLOCKS // QUARTERS, TILE, LANES), F32),
            pltpu.VMEM((BLOCKS, ROWS, LANES), F32),
            pltpu.VMEM((BLOCKS * ROWS, 2 * LANES), BF16),
            pltpu.VMEM((BLOCKS * ROWS, 2 * LANES), BF16),
            pltpu.VMEM((count * 8, LANES), F32),
            pltpu.SemaphoreType.DMA((len(operands),)),
        ]
        + [pltpu.SemaphoreType.DMA] * 8,
        compiler_params=pltpu.CompilerParams(
            collective_id=0, has_side_effects=True, vmem_limit_bytes=VMEM_LIMIT
        ),
    )(*operands)
    return pl.pallas_call(
        column_kernel,
        out_shape=jax.ShapeDtypeStruct((OUT_ROWS, G), F32),
        in_specs=[pl.BlockSpec(memory_space=pltpu.VMEM)] * 4,
        out_specs=pl.BlockSpec(memory_space=pl.ANY),
        scratch_shapes=[
            pltpu.VMEM((OUT_ROWS, G), F32),
            pltpu.SemaphoreType.DMA((BLOCKS * ROWS // LANES,)),
        ],
        compiler_params=pltpu.CompilerParams(vmem_limit_bytes=VMEM_LIMIT),
    )(columns, *constants[3:])


def solution(mesh):
    spec = P(("layout", "tile", "chan"), None, None)
    return jax.shard_map(
        body,
        mesh=mesh,
        in_specs=(spec,) * 5,
        out_specs=P(("layout", "tile", "chan"), None),
        check_vma=False,
    )
```
